32 devices in a mesh: sweep: 2 (over y), seq: 8 (over z, x), head: 2 (over core).
Axes of the slice: x: 2, y: 2, z: 4, core: 2. Of those that a mesh axis runs over, the one named last changes fastest.
Arguments:
- queries: bfloat16 [2048, 1024], P(('sweep', 'seq'), 'head'), parts along dimension 0, may hold values from -6 to 6
- key_matrix: bfloat16 [2048, 256], P(('sweep', 'seq'), 'head'), parts along dimension 0, may hold values from -6 to 6
- value_matrix: bfloat16 [2048, 256], P(('sweep', 'seq'), 'head'), parts along dimension 0, may hold values from -6 to 6
- segment_ids: int32 [2048], P(('sweep', 'seq')), parts along dimension 0, may hold values from 0 to 16, as said below
Outputs:
- attended: bfloat16 [2048, 1024], P(('sweep', 'seq'), 'head'), parts along dimension 0
The draws below stay inside these ranges and needn't reach their ends.
There are 2 independent parts, one for each index of `sweep`. The reference program is written for one: setup_inputs(seed, part) draws one part's arguments, and reference() takes and returns one part's arrays. A program takes and returns all parts, laid end to end along the dimension named above; each array names one. Nothing has to cross between parts.
Inputs may be any that keep to these rules, and one draw needn't show every extreme that they name: `segment_ids`: never falling. Segment 0 is a prompt at the start of 128 to 256 tokens; each id of 1 to 16 is one response of one or more tokens.
All inputs are finite; a program needn't handle non-finite values.
Results may differ from the reference program's by a relative error of at most 0.005.
Values may be sent and summed in bfloat16 or wider, within the bound.
No kernel may reach another device: no remote copies, remote signals or barrier semaphores. Data moves between devices by JAX's collectives and lax.ppermute only.
A program may use at most 64 MiB of HBM per device.

```python
import math
import jax
import jax.numpy as jnp
from jax import lax

QUERY_HEAD_COUNT = 16
KEY_VALUE_HEADS = 4
HEAD_WIDTH = 64
RESP = 16
TOKENS_PER_SHARD = 128
ROLLOUT_TOKENS = 1024
N_SEQ = 8


def draw_queries(key, part):
    base_offset = jnp.clip(jax.random.normal(jax.random.fold_in(key, 1), (ROLLOUT_TOKENS, QUERY_HEAD_COUNT * HEAD_WIDTH), jnp.float32), -6.0, 6.0)
    return base_offset.astype(jnp.bfloat16)


def draw_key_matrix(key, part):
    base_offset = jnp.clip(jax.random.normal(jax.random.fold_in(key, 2), (ROLLOUT_TOKENS, KEY_VALUE_HEADS * HEAD_WIDTH), jnp.float32), -6.0, 6.0)
    return base_offset.astype(jnp.bfloat16)


def draw_segment_ids(key, part):
    position = jnp.arange(ROLLOUT_TOKENS, dtype=jnp.int32)
    prompt = jax.random.randint(jax.random.fold_in(key, 21), (), ROLLOUT_TOKENS // 8, ROLLOUT_TOKENS // 4 + 1)
    later = jax.random.permutation(jax.random.fold_in(key, 22), jnp.arange(ROLLOUT_TOKENS // 4 + 1, ROLLOUT_TOKENS, dtype=jnp.int32))
    later = later[:RESP - 1]
    labels = (position >= prompt).astype(jnp.int32)
    labels = labels + jnp.sum((position[:, None] >= later[None, :]).astype(jnp.int32), axis=1)
    return labels.astype(jnp.int32)


def level_of(key, shape, cuts, low, high):
    gain = 1.0
    for axis_at, shards_of in cuts:
        steps = jax.random.uniform(jax.random.fold_in(jax.random.fold_in(key, 6), axis_at), (shards_of,), jnp.float32, low / len(cuts), high / len(cuts))
        gain = gain * jnp.repeat(jnp.exp(steps), shape[axis_at] // shards_of).reshape((-1,) + (1,) * (len(shape) - 1 - axis_at))
    return gain


def scatter_about(stream_key, extent, spread, most, pieces=(), held_as=jnp.bfloat16):
    gain = level_of(stream_key, extent, pieces, -0.22, 0.18) if pieces else 1.0
    values = jax.random.normal(stream_key, extent, jnp.float32) * spread * gain
    return jnp.minimum(jnp.maximum(values, -most), most).astype(held_as)


def setup_inputs(seed: int = 0, part: int = 0) -> dict:
    arg_keys = jax.random.split(jax.random.key(seed), 5)
    part_splits = jax.random.split(jax.random.fold_in(arg_keys[4], part), 5)
    return {
        "queries": draw_queries(jax.random.fold_in(jax.random.fold_in(arg_keys[4], part), 71), part),
        "key_matrix": draw_key_matrix(jax.random.fold_in(jax.random.fold_in(arg_keys[4], part), 71), part),
        "value_matrix": scatter_about(part_splits[2], (ROLLOUT_TOKENS, KEY_VALUE_HEADS * HEAD_WIDTH), 1.0, 6.0, ((0, 8), (1, 2))),
        "segment_ids": draw_segment_ids(jax.random.fold_in(jax.random.fold_in(arg_keys[4], part), 71), part),
    }


NEG_FILL = -1e+30

def reference(queries, key_matrix, value_matrix, segment_ids):
    repeat_factor = QUERY_HEAD_COUNT // KEY_VALUE_HEADS
    gathered_keys = key_matrix.reshape(ROLLOUT_TOKENS, KEY_VALUE_HEADS, HEAD_WIDTH).astype(jnp.float32)
    gathered_values = value_matrix.reshape(ROLLOUT_TOKENS, KEY_VALUE_HEADS, HEAD_WIDTH).astype(jnp.float32)
    key_pos = jnp.arange(ROLLOUT_TOKENS, dtype=jnp.int32)
    score_scale = 1.0 / math.sqrt(HEAD_WIDTH)

    def one_block(index):
        first = (index * TOKENS_PER_SHARD).astype(jnp.int32)
        query_block = lax.dynamic_slice_in_dim(queries, first, TOKENS_PER_SHARD, 0)
        query_block = query_block.reshape(TOKENS_PER_SHARD, KEY_VALUE_HEADS, repeat_factor, HEAD_WIDTH).astype(jnp.float32)
        query_seg = lax.dynamic_slice_in_dim(segment_ids, first, TOKENS_PER_SHARD, 0)
        query_pos = first + jnp.arange(TOKENS_PER_SHARD, dtype=jnp.int32)
        visible = (key_pos[None, :] <= query_pos[:, None]) & ((segment_ids[None, :] == query_seg[:, None]) | (segment_ids[None, :] == 0))
        logit_scores = jnp.einsum('opez,hpz->peoh', query_block, gathered_keys) * score_scale
        logit_scores = jnp.where(visible, logit_scores, NEG_FILL)
        top = lax.optimization_barrier(jnp.max(logit_scores, axis=-1, keepdims=True))
        weights = jnp.where(visible, jnp.exp(logit_scores - top), 0.0)
        weight_total = lax.optimization_barrier(jnp.sum(weights, axis=-1))
        rounded_scores = lax.optimization_barrier(weights.astype(jnp.bfloat16)).astype(jnp.float32)
        mixed_output = jnp.einsum('omhy,yoc->omhc', rounded_scores, gathered_values) / weight_total[..., None]
        result = jnp.transpose(mixed_output, (2, 0, 1, 3)).reshape(TOKENS_PER_SHARD, QUERY_HEAD_COUNT * HEAD_WIDTH)
        return result.astype(jnp.bfloat16)
    blocks = lax.map(one_block, jnp.arange(N_SEQ, dtype=jnp.int32))
    return blocks.reshape(ROLLOUT_TOKENS, QUERY_HEAD_COUNT * HEAD_WIDTH)
```

```python
import functools
import math

import jax
import jax.numpy as jnp
from jax import lax
from jax.experimental import pallas as pl
from jax.experimental.pallas import tpu as pltpu
from jax.sharding import PartitionSpec as P

HEAD_WIDTH = 64
NEG_FILL = -1e30
SEG_ROWS = 16


def attend_kernel(groups, repeat, count, *refs):
    q_ref, k_ref, v_ref, seg_ref = refs[:4]
    pieces = refs[4 : 3 + count]
    out_ref, q_all, scores = refs[3 + count :]
    tokens, lanes = k_ref.shape
    width = lanes // groups
    heads = groups * repeat
    factor = math.log2(math.e) / math.sqrt(width)
    me = lax.axis_index("seq")

    lane = lax.broadcasted_iota(jnp.int32, (tokens, lanes), 1)
    for head in range(heads):
        group = head // repeat
        first = head * width // lanes * lanes
        tile = q_ref[:, first : first + lanes].astype(jnp.float32)
        shift = (group * width - (head * width - first)) % lanes
        if shift:
            tile = pltpu.roll(tile, shift, 1)
        keep = (lane >= group * width) & (lane < (group + 1) * width)
        q_all[head * tokens : (head + 1) * tokens, :] = jnp.where(keep, tile, 0.0).astype(jnp.bfloat16)

    own_seg = seg_ref[...].astype(jnp.float32)
    query_seg = jnp.transpose(jnp.broadcast_to(own_seg, (tokens, tokens)))
    row = lax.broadcasted_iota(jnp.int32, (tokens, tokens), 0)
    col = lax.broadcasted_iota(jnp.int32, (tokens, tokens), 1)

    def bias_of(step):
        if step == 0:
            key_seg = jnp.broadcast_to(own_seg, (tokens, tokens))
            seen = ((key_seg == query_seg) | (key_seg == 0.0)) & (col <= row)
        else:
            key_row = pieces[step - 1][tokens : tokens + SEG_ROWS, :tokens].astype(jnp.float32)[0:1]
            key_seg = jnp.broadcast_to(key_row, (tokens, tokens))
            key_seg = jnp.where((me ^ step) < me, key_seg, -1.0)
            seen = (key_seg == query_seg) | (key_seg == 0.0)
        return jnp.where(seen, 0.0, NEG_FILL)

    def keys(step):
        return k_ref[...] if step == 0 else pieces[step - 1][:tokens, :lanes]

    def values(step):
        return v_ref[...] if step == 0 else pieces[step - 1][:tokens, lanes : 2 * lanes]

    blocks = count // 2
    query_rows = q_all[...]
    biases = []
    for block in range(blocks):
        key_block = jnp.concatenate([keys(2 * block), keys(2 * block + 1)], axis=0)
        scores[block] = lax.dot_general(
            query_rows, key_block, (((1,), (1,)), ((), ())), preferred_element_type=jnp.float32
        )
        biases.append(jnp.concatenate([bias_of(2 * block), bias_of(2 * block + 1)], axis=1))
    value_blocks = [
        jnp.concatenate([values(2 * block), values(2 * block + 1)], axis=0) for block in range(blocks)
    ]
    results = []
    for head in range(heads):
        rows = slice(head * tokens, (head + 1) * tokens)
        top = None
        masked = []
        for block in range(blocks):
            part = scores[block, rows, :] + biases[block]
            masked.append(part)
            high = jnp.maximum(part[:, :tokens], part[:, tokens:])
            top = high if top is None else jnp.maximum(top, high)
        top = jnp.max(top, axis=1, keepdims=True)
        mixed = total = None
        for block in range(blocks):
            weights = jnp.exp2((masked[block] - top) * factor)
            part = weights[:, :tokens] + weights[:, tokens:]
            total = part if total is None else total + part
            product = jnp.dot(
                weights.astype(jnp.bfloat16), value_blocks[block], preferred_element_type=jnp.float32
            )
            mixed = product if mixed is None else mixed + product
        results.append(mixed / jnp.sum(total, axis=1, keepdims=True))
    per_tile = lanes // width
    for tile in range(heads // per_tile):
        joined = None
        for slot in range(per_tile):
            head = tile * per_tile + slot
            shift = (slot * width - head // repeat * width) % lanes
            value = results[head]
            if shift:
                value = pltpu.roll(value, shift, 1)
            joined = value if joined is None else jnp.where(lane >= slot * width, value, joined)
        out_ref[:, tile * lanes : (tile + 1) * lanes] = joined.astype(jnp.bfloat16)


def per_device(count, queries, key_matrix, value_matrix, segment_ids):
    tokens, lanes = key_matrix.shape
    groups = lanes // HEAD_WIDTH
    repeat = queries.shape[1] // HEAD_WIDTH // groups
    heads = groups * repeat
    seg_row = jnp.pad(segment_ids.astype(jnp.bfloat16)[None], ((0, SEG_ROWS - 1), (0, 2 * lanes - tokens)))
    packed = jnp.concatenate([jnp.concatenate([key_matrix, value_matrix], axis=1), seg_row], axis=0)

    def exchange(array, step):
        return lax.ppermute(array, "seq", [(i, i ^ step) for i in range(count)])

    held = {0: packed}
    for step in range(2, count, 2):
        held[step] = exchange(packed, step)
    for step in range(0, count, 2):
        held[step + 1] = exchange(held[step], 1)
    pieces = [held[step] for step in range(1, count)]
    vmem = pl.BlockSpec(memory_space=pltpu.VMEM)
    return pl.pallas_call(
        functools.partial(attend_kernel, groups, repeat, count),
        out_shape=jax.ShapeDtypeStruct(queries.shape, queries.dtype),
        in_specs=[vmem] * (3 + count),
        out_specs=vmem,
        scratch_shapes=[
            pltpu.VMEM((heads * tokens, lanes), jnp.bfloat16),
            pltpu.VMEM((count // 2, heads * tokens, 2 * tokens), jnp.float32),
        ],
        name="attend",
    )(queries, key_matrix, value_matrix, segment_ids.reshape(1, tokens), *pieces)


def attend_block(state, query_heads, query_pos, query_seg, key_blk, value_blk, seg_blk, key_start):
    run_max, weight_total, totals = state
    groups = query_heads.shape[1]
    head_size = query_heads.shape[3]
    count = key_blk.shape[0]
    key_pos = key_start + jnp.arange(count, dtype=jnp.int32)
    visible = (key_pos[None, :] <= query_pos[:, None]) & (
        (seg_blk[None, :] == query_seg[:, None]) | (seg_blk[None, :] == 0)
    )

    def update(unused):
        logit_scores = jnp.einsum(
            "opez,hpz->peoh",
            query_heads,
            key_blk.reshape(count, groups, head_size),
            preferred_element_type=jnp.float32,
        ) * (1.0 / math.sqrt(head_size))
        logit_scores = jnp.where(visible, logit_scores, NEG_FILL)
        new_max = jnp.maximum(run_max, jnp.max(logit_scores, axis=-1))
        weights = jnp.where(visible, jnp.exp(logit_scores - new_max[..., None]), 0.0)
        rescale = jnp.exp(run_max - new_max)
        new_sum = weight_total * rescale + jnp.sum(weights, axis=-1)
        mixed_output = jnp.einsum(
            "omhy,yoc->omhc",
            weights.astype(jnp.bfloat16),
            value_blk.reshape(count, groups, head_size),
            preferred_element_type=jnp.float32,
        )
        return (new_max, new_sum, totals * rescale[..., None] + mixed_output)

    def keep(unused):
        return state

    return lax.cond(jnp.any(visible), update, keep, 0)


def build_fold(query_sets):

    def apply_all(states, key_piece, value_piece, seg_piece, start):
        return tuple(
            (
                attend_block(
                    states[number],
                    entry[0],
                    entry[1],
                    entry[2],
                    key_piece,
                    value_piece,
                    seg_piece,
                    start,
                )
                for number, entry in enumerate(query_sets)
            )
        )

    def fold(states, piece, start):
        key_piece, value_piece, seg_piece = piece
        rows = key_piece.shape[0]
        width = 512

        def loop_step(index, carried):
            offset = index * width
            return apply_all(
                carried,
                lax.dynamic_slice_in_dim(key_piece, offset, width, 0),
                lax.dynamic_slice_in_dim(value_piece, offset, width, 0),
                lax.dynamic_slice_in_dim(seg_piece, offset, width, 0),
                offset,
            )

        return lax.fori_loop(0, rows // width, loop_step, states)

    return fold


def start_state(query_heads):
    tok_rows, groups, repeat_factor, head_size = query_heads.shape
    return (
        jnp.full((groups, repeat_factor, tok_rows), NEG_FILL, jnp.float32),
        jnp.zeros((groups, repeat_factor, tok_rows), jnp.float32),
        jnp.zeros((groups, repeat_factor, tok_rows, head_size), jnp.float32),
    )


def finish(state):
    run_max, weight_total, totals = state
    result = totals / weight_total[..., None]
    groups, repeat_factor, tok_rows, head_size = result.shape
    return (
        jnp.transpose(result, (2, 0, 1, 3))
        .reshape(tok_rows, groups * repeat_factor * head_size)
        .astype(jnp.bfloat16)
    )


def per_device_general(queries, key_matrix, value_matrix, segment_ids):
    head_size = HEAD_WIDTH
    block_rows = segment_ids.shape[0]
    groups = key_matrix.shape[1] // head_size
    repeat_factor = queries.shape[1] // head_size // groups
    position = lax.axis_index("seq")
    query_pos = position * block_rows + jnp.arange(block_rows, dtype=jnp.int32)
    query_sets = (
        (queries.reshape(block_rows, groups, repeat_factor, head_size), query_pos, segment_ids),
    )
    fold = build_fold(query_sets)
    states = tuple((start_state(entry[0]) for entry in query_sets))
    states = fold(
        states,
        (
            lax.all_gather(key_matrix, "seq", axis=0, tiled=True),
            lax.all_gather(value_matrix, "seq", axis=0, tiled=True),
            lax.all_gather(segment_ids, "seq", axis=0, tiled=True),
        ),
        jnp.int32(0),
    )
    return finish(states[0])


def suits(count, queries, key_matrix):
    tokens, lanes = key_matrix.shape
    return (
        2 <= count <= 16
        and count & (count - 1) == 0
        and tokens == lanes == 2 * HEAD_WIDTH
        and queries.shape[1] % lanes == 0
    )


def per_device_any(count, queries, key_matrix, value_matrix, segment_ids):
    body = functools.partial(per_device, count)
    if not suits(count, queries, key_matrix):
        body = per_device_general
    return body(queries, key_matrix, value_matrix, segment_ids)


def solution(mesh):
    count = mesh.shape["seq"]
    in_specs = (P(("sweep", "seq"), "head"),) * 3 + (P(("sweep", "seq")),)
    return jax.shard_map(
        functools.partial(per_device_any, count),
        mesh=mesh, in_specs=in_specs, out_specs=P(("sweep", "seq"), "head"), check_vma=False,
    )
```

```python
import functools
import math

import jax
import jax.numpy as jnp
from jax import lax
from jax.experimental import pallas as pl
from jax.experimental.pallas import tpu as pltpu
from jax.sharding import PartitionSpec as P


HEAD_WIDTH = 64
NEG_FILL = -1e30
SEG_ROWS = 8
SMALL_VMEM = 1 << 20
VMEM_LIMIT = 16 << 20
VMEM = pl.BlockSpec(memory_space=pltpu.VMEM)
HBM = pl.BlockSpec(memory_space=pltpu.HBM)


def in_hbm(array):
    return pltpu.with_memory_space_constraint(array, pltpu.HBM)


def pack_kernel(k_ref, v_ref, seg_ref, out_ref, seg_buf, sems):
    tokens, lanes = k_ref.shape
    copies = [
        pltpu.make_async_copy(seg_ref, seg_buf, sems.at[0]),
        pltpu.make_async_copy(k_ref, out_ref.at[:tokens, :lanes], sems.at[1]),
        pltpu.make_async_copy(v_ref, out_ref.at[:tokens, lanes:], sems.at[2]),
    ]
    for copy in copies:
        copy.start()
    copies[0].wait()
    row = jnp.broadcast_to(seg_buf[...].astype(jnp.float32), (SEG_ROWS, tokens)).astype(jnp.bfloat16)
    out_ref[tokens:, :lanes] = row
    out_ref[tokens:, lanes:] = row
    copies[1].wait()
    copies[2].wait()


def pack(key_matrix, value_matrix, seg_row):
    tokens, lanes = key_matrix.shape
    return pl.pallas_call(
        pack_kernel,
        out_shape=pltpu.VMEM((tokens + SEG_ROWS, 2 * lanes), key_matrix.dtype),
        in_specs=[HBM] * 3,
        out_specs=VMEM,
        scratch_shapes=[pltpu.VMEM((1, tokens), jnp.int32), pltpu.SemaphoreType.DMA((3,))],
        compiler_params=pltpu.CompilerParams(vmem_limit_bytes=SMALL_VMEM),
        name="pack",
    )(in_hbm(key_matrix), in_hbm(value_matrix), in_hbm(seg_row))


def joined(pieces, first, width, tokens):
    parts = [piece[:tokens, first : first + width] for piece in pieces]
    return parts[0] if len(parts) == 1 else jnp.concatenate(parts, axis=0)


def seg_grid(piece, tokens):
    line = piece[tokens : tokens + SEG_ROWS, :tokens].astype(jnp.float32)[0:1]
    return jnp.broadcast_to(line, (tokens, tokens))


def bias_of(me, step, piece, query_seg):
    tokens = query_seg.shape[0]
    key_seg = seg_grid(piece, tokens)
    if step == 0:
        row = lax.broadcasted_iota(jnp.int32, (tokens, tokens), 0)
        col = lax.broadcasted_iota(jnp.int32, (tokens, tokens), 1)
        seen = ((key_seg == query_seg) | (key_seg == 0.0)) & (col <= row)
    else:
        if step == 1:
            key_seg = jnp.where((me ^ step) < me, key_seg, -1.0)
        seen = (key_seg == query_seg) | (key_seg == 0.0)
    return jnp.where(seen, 0.0, NEG_FILL)


def folded(values, tokens, op):
    parts = [values[:, at : at + tokens] for at in range(0, values.shape[1], tokens)]
    return functools.reduce(op, parts)


def attend(me, blocks, query_seg, q_all, scores, heads, factor, lanes, before, after):
    tokens = query_seg.shape[0]
    query_rows = q_all[...]
    biases, value_blocks = [], []
    for number, block in enumerate(blocks):
        members = [piece for _, piece in block]
        scores[number, :, : len(block) * tokens] = lax.dot_general(
            query_rows, joined(members, 0, lanes, tokens), (((1,), (1,)), ((), ())),
            preferred_element_type=jnp.float32,
        )
        parts = [bias_of(me, step, piece, query_seg) for step, piece in block]
        biases.append(parts[0] if len(parts) == 1 else jnp.concatenate(parts, axis=1))
        value_blocks.append(joined(members, lanes, lanes, tokens))
    for head in range(heads):
        rows = slice(head * tokens, (head + 1) * tokens)
        state = before(rows)
        masked = []
        high = None if state is None else state[0]
        for number, block in enumerate(blocks):
            part = scores[number, rows, : len(block) * tokens] + biases[number]
            masked.append(part)
            part = folded(part, tokens, jnp.maximum)
            high = part if high is None else jnp.maximum(high, part)
        top = jnp.max(high, axis=1, keepdims=True)
        total = mixed = None
        if state is not None:
            rescale = jnp.exp2((state[0] - top) * factor)
            total, mixed = state[1] * rescale, state[2] * rescale
        for part, value_block in zip(masked, value_blocks):
            weights = jnp.exp2((part - top) * factor)
            share = folded(weights, tokens, jnp.add)
            total = share if total is None else total + share
            product = jnp.dot(
                weights.astype(jnp.bfloat16), value_block, preferred_element_type=jnp.float32
            )
            mixed = product if mixed is None else mixed + product
        after(head, rows, top, total, mixed)


def assemble(results, repeat, width, lanes, out_buf):
    tokens = out_buf.shape[0]
    lane = lax.broadcasted_iota(jnp.int32, (tokens, lanes), 1)
    per_tile = lanes // width
    for tile in range(len(results) // per_tile):
        whole = None
        for slot in range(per_tile):
            head = tile * per_tile + slot
            shift = (slot * width - head // repeat * width) % lanes
            value = results[head]
            if shift:
                value = pltpu.roll(value, shift, 1)
            whole = value if whole is None else jnp.where(lane >= slot * width, value, whole)
        out_buf[:, tile * lanes : (tile + 1) * lanes] = whole.astype(jnp.bfloat16)


def normal(total, mixed):
    return mixed * (1.0 / jnp.sum(total, axis=1, keepdims=True))


def paired(items):
    return [items[at : at + 2] for at in range(0, len(items), 2)]


def seen_steps(pair, count):
    return [step for step in range(2, count, 2) if pair ^ (step >> 1) < pair]


def near_kernel(groups, repeat, count, *refs):
    steps = [0, 1] + list(range(2, count, 2))
    q_hbm, pieces = refs[0], dict(zip(steps, refs[1 : 1 + len(steps)]))
    q_all, seg_ref, top_ref, sum_ref, mix_ref, out_hbm, q_buf, scores, sem = refs[1 + len(steps) :]
    tokens, _ = q_buf.shape
    lanes = q_all.shape[1]
    width = lanes // groups
    heads = groups * repeat
    factor = math.log2(math.e) / math.sqrt(width)
    me = lax.axis_index("seq")

    copy = pltpu.make_async_copy(q_hbm, q_buf, sem)
    copy.start()
    query_seg = jnp.transpose(seg_grid(pieces[0], tokens))
    seg_ref[...] = query_seg
    lane = lax.broadcasted_iota(jnp.int32, (tokens, lanes), 1)
    copy.wait()
    for head in range(heads):
        group = head // repeat
        first = head * width // lanes * lanes
        tile = q_buf[:, first : first + lanes].astype(jnp.float32)
        shift = (group * width - (head * width - first)) % lanes
        if shift:
            tile = pltpu.roll(tile, shift, 1)
        keep = (lane >= group * width) & (lane < (group + 1) * width)
        q_all[head * tokens : (head + 1) * tokens, :] = jnp.where(keep, tile, 0.0).astype(jnp.bfloat16)

    for pair in range(count // 2):

        @pl.when(me // 2 == pair)
        def _(pair=pair):
            early = seen_steps(pair, count)
            chosen = [0, 1] + early[len(early) % 2 :] + early[: len(early) % 2]
            blocks = paired([(step, pieces[step]) for step in chosen])
            results = []

            def after(head, rows, top, total, mixed):
                if early:
                    top_ref[rows, :] = jnp.broadcast_to(top, (tokens, lanes))
                    sum_ref[rows, :] = total
                    mix_ref[rows, :] = mixed
                else:
                    results.append(normal(total, mixed))

            attend(me, blocks, query_seg, q_all, scores, heads, factor, lanes, lambda rows: None, after)
            if not early:
                assemble(results, repeat, width, lanes, q_buf)
                out_copy = pltpu.make_async_copy(q_buf, out_hbm, sem)
                out_copy.start()
                out_copy.wait()


def far_kernel(groups, repeat, count, *refs):
    steps = list(range(3, count, 2))
    q_all, seg_ref, top_ref, sum_ref, mix_ref, out_in = refs[:6]
    pieces = dict(zip(steps, refs[6 : 6 + len(steps)]))
    out_hbm, out_buf, scores, sem = refs[6 + len(steps) :]
    del out_in
    lanes = q_all.shape[1]
    width = lanes // groups
    heads = groups * repeat
    factor = math.log2(math.e) / math.sqrt(width)
    me = lax.axis_index("seq")

    for pair in range(1, count // 2):

        @pl.when(me // 2 == pair)
        def _(pair=pair):
            blocks = paired([(step + 1, pieces[step + 1]) for step in seen_steps(pair, count)])
            results = []

            def before(rows):
                return top_ref[rows, :], sum_ref[rows, :], mix_ref[rows, :]

            def after(head, rows, top, total, mixed):
                results.append(normal(total, mixed))

            attend(me, blocks, seg_ref[...], q_all, scores, heads, factor, lanes, before, after)
            assemble(results, repeat, width, lanes, out_buf)
            out_copy = pltpu.make_async_copy(out_buf, out_hbm, sem)
            out_copy.start()
            out_copy.wait()


def plan_of(count):
    powers = [1 << bit for bit in range(1, count.bit_length() - 1)]
    plan = [(step, 0, step) for step in reversed(powers)] + [(1, 0, 1)]
    for step in range(2, count, 2):
        if step not in powers:
            low = step & -step
            plan.append((step, step ^ low, low))
    plan += [(step + 1, step, 1) for step in range(2, count, 2)]
    return plan


def per_device(count, queries, key_matrix, value_matrix, segment_ids):
    tokens, lanes = key_matrix.shape
    groups = lanes // HEAD_WIDTH
    repeat = queries.shape[1] // HEAD_WIDTH // groups
    heads = groups * repeat
    plan = plan_of(count)
    held = {0: pack(key_matrix, value_matrix, segment_ids.reshape(1, tokens))}
    for step, source, mask in plan:
        held[step] = lax.ppermute(held[source], "seq", [(i, i ^ mask) for i in range(count)])
    near = [0, 1] + list(range(2, count, 2))
    far = list(range(3, count, 2))
    row_shape = (heads * tokens, lanes)
    score_shape = (heads * tokens, 2 * tokens)
    *state, out = pl.pallas_call(
        functools.partial(near_kernel, groups, repeat, count),
        out_shape=[
            pltpu.VMEM(row_shape, jnp.bfloat16),
            pltpu.VMEM((tokens, tokens), jnp.float32),
            pltpu.VMEM(row_shape, jnp.float32),
            pltpu.VMEM(row_shape, jnp.float32),
            pltpu.VMEM(row_shape, jnp.float32),
            pltpu.HBM(queries.shape, queries.dtype),
        ],
        in_specs=[HBM] + [VMEM] * len(near),
        out_specs=[VMEM] * 5 + [HBM],
        scratch_shapes=[
            pltpu.VMEM(queries.shape, queries.dtype),
            pltpu.VMEM(((len(near) + 1) // 2,) + score_shape, jnp.float32),
            pltpu.SemaphoreType.DMA,
        ],
        compiler_params=pltpu.CompilerParams(vmem_limit_bytes=VMEM_LIMIT),
        name="near",
    )(in_hbm(queries), *[held[step] for step in near])
    return pl.pallas_call(
        functools.partial(far_kernel, groups, repeat, count),
        out_shape=pltpu.HBM(queries.shape, queries.dtype),
        in_specs=[VMEM] * 5 + [HBM] + [VMEM] * len(far),
        out_specs=HBM,
        scratch_shapes=[
            pltpu.VMEM(queries.shape, queries.dtype),
            pltpu.VMEM(((len(far) + 1) // 2,) + score_shape, jnp.float32),
            pltpu.SemaphoreType.DMA,
        ],
        input_output_aliases={5: 0},
        compiler_params=pltpu.CompilerParams(vmem_limit_bytes=VMEM_LIMIT),
        name="far",
    )(*state, out, *[held[step] for step in far])


def attend_block(state, query_heads, query_pos, query_seg, key_blk, value_blk, seg_blk, key_start):
    run_max, weight_total, totals = state
    groups = query_heads.shape[1]
    head_size = query_heads.shape[3]
    count = key_blk.shape[0]
    key_pos = key_start + jnp.arange(count, dtype=jnp.int32)
    visible = (key_pos[None, :] <= query_pos[:, None]) & (
        (seg_blk[None, :] == query_seg[:, None]) | (seg_blk[None, :] == 0)
    )

    def update(unused):
        logit_scores = jnp.einsum(
            "opez,hpz->peoh",
            query_heads,
            key_blk.reshape(count, groups, head_size),
            preferred_element_type=jnp.float32,
        ) * (1.0 / math.sqrt(head_size))
        logit_scores = jnp.where(visible, logit_scores, NEG_FILL)
        new_max = jnp.maximum(run_max, jnp.max(logit_scores, axis=-1))
        weights = jnp.where(visible, jnp.exp(logit_scores - new_max[..., None]), 0.0)
        rescale = jnp.exp(run_max - new_max)
        new_sum = weight_total * rescale + jnp.sum(weights, axis=-1)
        mixed_output = jnp.einsum(
            "omhy,yoc->omhc",
            weights.astype(jnp.bfloat16),
            value_blk.reshape(count, groups, head_size),
            preferred_element_type=jnp.float32,
        )
        return (new_max, new_sum, totals * rescale[..., None] + mixed_output)

    def keep(unused):
        return state

    return lax.cond(jnp.any(visible), update, keep, 0)


def build_fold(query_sets):

    def apply_all(states, key_piece, value_piece, seg_piece, start):
        return tuple(
            (
                attend_block(
                    states[number],
                    entry[0],
                    entry[1],
                    entry[2],
                    key_piece,
                    value_piece,
                    seg_piece,
                    start,
                )
                for number, entry in enumerate(query_sets)
            )
        )

    def fold(states, piece, start):
        key_piece, value_piece, seg_piece = piece
        rows = key_piece.shape[0]
        width = 512

        def loop_step(index, carried):
            offset = index * width
            return apply_all(
                carried,
                lax.dynamic_slice_in_dim(key_piece, offset, width, 0),
                lax.dynamic_slice_in_dim(value_piece, offset, width, 0),
                lax.dynamic_slice_in_dim(seg_piece, offset, width, 0),
                offset,
            )

        return lax.fori_loop(0, rows // width, loop_step, states)

    return fold


def start_state(query_heads):
    tok_rows, groups, repeat_factor, head_size = query_heads.shape
    return (
        jnp.full((groups, repeat_factor, tok_rows), NEG_FILL, jnp.float32),
        jnp.zeros((groups, repeat_factor, tok_rows), jnp.float32),
        jnp.zeros((groups, repeat_factor, tok_rows, head_size), jnp.float32),
    )


def finish(state):
    _, weight_total, totals = state
    result = totals / weight_total[..., None]
    groups, repeat_factor, tok_rows, head_size = result.shape
    return (
        jnp.transpose(result, (2, 0, 1, 3))
        .reshape(tok_rows, groups * repeat_factor * head_size)
        .astype(jnp.bfloat16)
    )


def per_device_general(queries, key_matrix, value_matrix, segment_ids):
    head_size = HEAD_WIDTH
    block_rows = segment_ids.shape[0]
    groups = key_matrix.shape[1] // head_size
    repeat_factor = queries.shape[1] // head_size // groups
    position = lax.axis_index("seq")
    query_pos = position * block_rows + jnp.arange(block_rows, dtype=jnp.int32)
    query_sets = (
        (queries.reshape(block_rows, groups, repeat_factor, head_size), query_pos, segment_ids),
    )
    fold = build_fold(query_sets)
    states = tuple((start_state(entry[0]) for entry in query_sets))
    states = fold(
        states,
        (
            lax.all_gather(key_matrix, "seq", axis=0, tiled=True),
            lax.all_gather(value_matrix, "seq", axis=0, tiled=True),
            lax.all_gather(segment_ids, "seq", axis=0, tiled=True),
        ),
        jnp.int32(0),
    )
    return finish(states[0])


def paired_axis(count):
    return 8 <= count <= 16 and count & (count - 1) == 0


def suits(count, queries, key_matrix):
    tokens, lanes = key_matrix.shape
    return (
        paired_axis(count)
        and tokens == lanes == 2 * HEAD_WIDTH
        and queries.shape[1] % lanes == 0
    )


def per_device_any(count, queries, key_matrix, value_matrix, segment_ids):
    body = functools.partial(per_device, count)
    if not suits(count, queries, key_matrix):
        body = per_device_general
    return body(queries, key_matrix, value_matrix, segment_ids)


def solution(mesh):
    count = mesh.shape["seq"]
    in_specs = (P(("sweep", "seq"), "head"),) * 3 + (P(("sweep", "seq")),)
    return jax.shard_map(
        functools.partial(per_device_any, count),
        mesh=mesh, in_specs=in_specs, out_specs=P(("sweep", "seq"), "head"), check_vma=False,
    )
```

```python
import functools
import math

import jax
import jax.numpy as jnp
from jax import lax
from jax.experimental import pallas as pl
from jax.experimental.pallas import tpu as pltpu
from jax.sharding import PartitionSpec as P


HEAD_WIDTH = 64
NEG_FILL = -1e30
SEG_ROWS = 8
SMALL_VMEM = 1 << 20
VMEM_LIMIT = 16 << 20
VMEM = pl.BlockSpec(memory_space=pltpu.VMEM)
HBM = pl.BlockSpec(memory_space=pltpu.HBM)


def in_hbm(array):
    return pltpu.with_memory_space_constraint(array, pltpu.HBM)


def pack_kernel(k_ref, v_ref, seg_ref, out_ref, seg_buf, sems):
    tokens, lanes = k_ref.shape
    copies = [
        pltpu.make_async_copy(seg_ref, seg_buf, sems.at[0]),
        pltpu.make_async_copy(k_ref, out_ref.at[:tokens, :lanes], sems.at[1]),
        pltpu.make_async_copy(v_ref, out_ref.at[:tokens, lanes:], sems.at[2]),
    ]
    for copy in copies:
        copy.start()
    copies[0].wait()
    row = jnp.broadcast_to(seg_buf[...].astype(jnp.float32), (SEG_ROWS, tokens)).astype(jnp.bfloat16)
    out_ref[tokens:, :lanes] = row
    out_ref[tokens:, lanes:] = row
    copies[1].wait()
    copies[2].wait()


def pack(key_matrix, value_matrix, seg_row):
    tokens, lanes = key_matrix.shape
    return pl.pallas_call(
        pack_kernel,
        out_shape=pltpu.VMEM((tokens + SEG_ROWS, 2 * lanes), key_matrix.dtype),
        in_specs=[HBM] * 3,
        out_specs=VMEM,
        scratch_shapes=[pltpu.VMEM((1, tokens), jnp.int32), pltpu.SemaphoreType.DMA((3,))],
        compiler_params=pltpu.CompilerParams(vmem_limit_bytes=SMALL_VMEM),
        name="pack",
    )(in_hbm(key_matrix), in_hbm(value_matrix), in_hbm(seg_row))


def joined(pieces, first, width, tokens):
    parts = [piece[:tokens, first : first + width] for piece in pieces]
    return parts[0] if len(parts) == 1 else jnp.concatenate(parts, axis=0)


def seg_grid(piece, tokens):
    line = piece[tokens : tokens + SEG_ROWS, :tokens].astype(jnp.float32)[0:1]
    return jnp.broadcast_to(line, (tokens, tokens))


def bias_of(me, step, piece, query_seg):
    tokens = query_seg.shape[0]
    key_seg = seg_grid(piece, tokens)
    if step == 0:
        row = lax.broadcasted_iota(jnp.int32, (tokens, tokens), 0)
        col = lax.broadcasted_iota(jnp.int32, (tokens, tokens), 1)
        seen = ((key_seg == query_seg) | (key_seg == 0.0)) & (col <= row)
    else:
        if step == 1:
            key_seg = jnp.where((me ^ step) < me, key_seg, -1.0)
        seen = (key_seg == query_seg) | (key_seg == 0.0)
    return jnp.where(seen, 0.0, NEG_FILL)


def folded(values, tokens, op):
    parts = [values[:, at : at + tokens] for at in range(0, values.shape[1], tokens)]
    return functools.reduce(op, parts)


def attend(me, blocks, query_seg, q_all, scores, heads, factor, lanes, before, after):
    tokens = query_seg.shape[0]
    query_rows = q_all[...]
    biases, value_blocks = [], []
    for number, block in enumerate(blocks):
        members = [piece for _, piece in block]
        scores[number, :, : len(block) * tokens] = lax.dot_general(
            query_rows, joined(members, 0, lanes, tokens), (((1,), (1,)), ((), ())),
            preferred_element_type=jnp.float32,
        )
        parts = [bias_of(me, step, piece, query_seg) for step, piece in block]
        biases.append(parts[0] if len(parts) == 1 else jnp.concatenate(parts, axis=1))
        value_blocks.append(joined(members, lanes, lanes, tokens))
    for head in range(heads):
        rows = slice(head * tokens, (head + 1) * tokens)
        state = before(rows)
        masked = []
        high = None if state is None else state[0]
        for number, block in enumerate(blocks):
            part = scores[number, rows, : len(block) * tokens] + biases[number]
            masked.append(part)
            part = folded(part, tokens, jnp.maximum)
            high = part if high is None else jnp.maximum(high, part)
        top = jnp.max(high, axis=1, keepdims=True)
        total = mixed = None
        if state is not None:
            rescale = jnp.exp2((state[0] - top) * factor)
            total, mixed = state[1] * rescale, state[2] * rescale
        for part, value_block in zip(masked, value_blocks):
            weights = jnp.exp2((part - top) * factor)
            share = folded(weights, tokens, jnp.add)
            total = share if total is None else total + share
            product = jnp.dot(
                weights.astype(jnp.bfloat16), value_block, preferred_element_type=jnp.float32
            )
            mixed = product if mixed is None else mixed + product
        after(head, rows, top, total, mixed)


class Output:
    def __init__(self, repeat, width, lanes, buf, hbm, sems):
        self.repeat, self.width, self.lanes = repeat, width, lanes
        self.buf, self.hbm, self.sems = buf, hbm, sems
        self.head, self.whole, self.copies = 0, None, []

    def add(self, value):
        slot = self.head % (self.lanes // self.width)
        shift = (slot * self.width - self.head // self.repeat * self.width) % self.lanes
        if shift:
            value = pltpu.roll(value, shift, 1)
        if slot:
            lane = lax.broadcasted_iota(jnp.int32, value.shape, 1)
            value = jnp.where(lane >= slot * self.width, value, self.whole)
        self.whole = value
        self.head += 1
        if (slot + 1) * self.width == self.lanes:
            tile = len(self.copies)
            where = slice(tile * self.lanes, (tile + 1) * self.lanes)
            self.buf[:, where] = value.astype(jnp.bfloat16)
            copy = pltpu.make_async_copy(self.buf.at[:, where], self.hbm.at[:, where], self.sems.at[tile])
            copy.start()
            self.copies.append(copy)

    def finish(self):
        for copy in self.copies:
            copy.wait()


def normal(total, mixed):
    return mixed * (1.0 / jnp.sum(total, axis=1, keepdims=True))


def paired(items):
    return [items[at : at + 2] for at in range(0, len(items), 2)]


def seen_steps(pair, count):
    return [step for step in range(2, count, 2) if pair ^ (step >> 1) < pair]


def prep_kernel(groups, repeat, q_hbm, own, q_all, seg_ref, q_buf, sems):
    tokens, columns = q_buf.shape
    lanes = q_all.shape[1]
    width = lanes // groups
    copies = [
        pltpu.make_async_copy(q_hbm.at[:, at : at + lanes], q_buf.at[:, at : at + lanes], sems.at[at // lanes])
        for at in range(0, columns, lanes)
    ]
    for copy in copies:
        copy.start()
    seg_ref[...] = jnp.transpose(seg_grid(own, tokens))
    lane = lax.broadcasted_iota(jnp.int32, (tokens, lanes), 1)
    for head in range(groups * repeat):
        group = head // repeat
        first = head * width // lanes * lanes
        if first == head * width:
            copies[first // lanes].wait()
        tile = q_buf[:, first : first + lanes].astype(jnp.float32)
        shift = (group * width - (head * width - first)) % lanes
        if shift:
            tile = pltpu.roll(tile, shift, 1)
        keep = (lane >= group * width) & (lane < (group + 1) * width)
        q_all[head * tokens : (head + 1) * tokens, :] = jnp.where(keep, tile, 0.0).astype(jnp.bfloat16)


def near_kernel(groups, repeat, count, *refs):
    steps = [0, 1] + list(range(2, count, 2))
    q_all, seg_ref, pieces = refs[0], refs[1], dict(zip(steps, refs[2 : 2 + len(steps)]))
    top_ref, sum_ref, mix_ref, out_hbm, out_buf, scores, sems = refs[2 + len(steps) :]
    lanes = q_all.shape[1]
    tokens = seg_ref.shape[0]
    width = lanes // groups
    heads = groups * repeat
    factor = math.log2(math.e) / math.sqrt(width)
    me = lax.axis_index("seq")
    query_seg = seg_ref[...]

    for pair in range(count // 2):

        @pl.when(me // 2 == pair)
        def _(pair=pair):
            early = seen_steps(pair, count)
            chosen = [0, 1] + early[len(early) % 2 :] + early[: len(early) % 2]
            blocks = paired([(step, pieces[step]) for step in chosen])
            output = Output(repeat, width, lanes, out_buf, out_hbm, sems)

            def after(head, rows, top, total, mixed):
                if early:
                    top_ref[rows, :] = jnp.broadcast_to(top, (tokens, lanes))
                    sum_ref[rows, :] = total
                    mix_ref[rows, :] = mixed
                else:
                    output.add(normal(total, mixed))

            attend(me, blocks, query_seg, q_all, scores, heads, factor, lanes, lambda rows: None, after)
            output.finish()


def far_kernel(groups, repeat, count, *refs):
    steps = list(range(3, count, 2))
    q_all, seg_ref, top_ref, sum_ref, mix_ref, out_in = refs[:6]
    pieces = dict(zip(steps, refs[6 : 6 + len(steps)]))
    out_hbm, out_buf, scores, sems = refs[6 + len(steps) :]
    del out_in
    lanes = q_all.shape[1]
    width = lanes // groups
    heads = groups * repeat
    factor = math.log2(math.e) / math.sqrt(width)
    me = lax.axis_index("seq")

    for pair in range(1, count // 2):

        @pl.when(me // 2 == pair)
        def _(pair=pair):
            blocks = paired([(step + 1, pieces[step + 1]) for step in seen_steps(pair, count)])
            output = Output(repeat, width, lanes, out_buf, out_hbm, sems)

            def before(rows):
                return top_ref[rows, :], sum_ref[rows, :], mix_ref[rows, :]

            def after(head, rows, top, total, mixed):
                output.add(normal(total, mixed))

            attend(me, blocks, seg_ref[...], q_all, scores, heads, factor, lanes, before, after)
            output.finish()


def plan_of(count):
    column = [count - 2] + list(range(2, count - 2, 2))
    return [(step, 0, step) for step in column] + [(1, 0, 1)] + [(step + 1, step, 1) for step in column]


def per_device(count, queries, key_matrix, value_matrix, segment_ids):
    tokens, lanes = key_matrix.shape
    groups = lanes // HEAD_WIDTH
    repeat = queries.shape[1] // HEAD_WIDTH // groups
    heads = groups * repeat
    plan = plan_of(count)
    held = {0: pack(key_matrix, value_matrix, segment_ids.reshape(1, tokens))}
    for step, source, mask in plan:
        held[step] = lax.ppermute(held[source], "seq", [(i, i ^ mask) for i in range(count)])
    near = [0, 1] + list(range(2, count, 2))
    far = list(range(3, count, 2))
    row_shape = (heads * tokens, lanes)
    score_shape = (heads * tokens, 2 * tokens)
    tiles = queries.shape[1] // lanes
    q_all, query_seg = pl.pallas_call(
        functools.partial(prep_kernel, groups, repeat),
        out_shape=[
            pltpu.VMEM(row_shape, jnp.bfloat16),
            pltpu.VMEM((tokens, tokens), jnp.float32),
        ],
        in_specs=[HBM, VMEM],
        out_specs=[VMEM] * 2,
        scratch_shapes=[
            pltpu.VMEM(queries.shape, queries.dtype),
            pltpu.SemaphoreType.DMA((tiles,)),
        ],
        compiler_params=pltpu.CompilerParams(vmem_limit_bytes=SMALL_VMEM),
        name="prep",
    )(in_hbm(queries), held[0])
    top, total, mixed, out = pl.pallas_call(
        functools.partial(near_kernel, groups, repeat, count),
        out_shape=[
            pltpu.VMEM(row_shape, jnp.float32),
            pltpu.VMEM(row_shape, jnp.float32),
            pltpu.VMEM(row_shape, jnp.float32),
            pltpu.HBM(queries.shape, queries.dtype),
        ],
        in_specs=[VMEM] * (2 + len(near)),
        out_specs=[VMEM] * 3 + [HBM],
        scratch_shapes=[
            pltpu.VMEM(queries.shape, queries.dtype),
            pltpu.VMEM(((len(near) + 1) // 2,) + score_shape, jnp.float32),
            pltpu.SemaphoreType.DMA((tiles,)),
        ],
        compiler_params=pltpu.CompilerParams(vmem_limit_bytes=VMEM_LIMIT),
        name="near",
    )(q_all, query_seg, *[held[step] for step in near])
    return pl.pallas_call(
        functools.partial(far_kernel, groups, repeat, count),
        out_shape=pltpu.HBM(queries.shape, queries.dtype),
        in_specs=[VMEM] * 5 + [HBM] + [VMEM] * len(far),
        out_specs=HBM,
        scratch_shapes=[
            pltpu.VMEM(queries.shape, queries.dtype),
            pltpu.VMEM(((len(far) + 1) // 2,) + score_shape, jnp.float32),
            pltpu.SemaphoreType.DMA((tiles,)),
        ],
        input_output_aliases={5: 0},
        compiler_params=pltpu.CompilerParams(vmem_limit_bytes=VMEM_LIMIT),
        name="far",
    )(q_all, query_seg, top, total, mixed, out, *[held[step] for step in far])


def attend_block(state, query_heads, query_pos, query_seg, key_blk, value_blk, seg_blk, key_start):
    run_max, weight_total, totals = state
    groups = query_heads.shape[1]
    head_size = query_heads.shape[3]
    count = key_blk.shape[0]
    key_pos = key_start + jnp.arange(count, dtype=jnp.int32)
    visible = (key_pos[None, :] <= query_pos[:, None]) & (
        (seg_blk[None, :] == query_seg[:, None]) | (seg_blk[None, :] == 0)
    )

    def update(unused):
        logit_scores = jnp.einsum(
            "opez,hpz->peoh",
            query_heads,
            key_blk.reshape(count, groups, head_size),
            preferred_element_type=jnp.float32,
        ) * (1.0 / math.sqrt(head_size))
        logit_scores = jnp.where(visible, logit_scores, NEG_FILL)
        new_max = jnp.maximum(run_max, jnp.max(logit_scores, axis=-1))
        weights = jnp.where(visible, jnp.exp(logit_scores - new_max[..., None]), 0.0)
        rescale = jnp.exp(run_max - new_max)
        new_sum = weight_total * rescale + jnp.sum(weights, axis=-1)
        mixed_output = jnp.einsum(
            "omhy,yoc->omhc",
            weights.astype(jnp.bfloat16),
            value_blk.reshape(count, groups, head_size),
            preferred_element_type=jnp.float32,
        )
        return (new_max, new_sum, totals * rescale[..., None] + mixed_output)

    def keep(unused):
        return state

    return lax.cond(jnp.any(visible), update, keep, 0)


def build_fold(query_sets):

    def apply_all(states, key_piece, value_piece, seg_piece, start):
        return tuple(
            (
                attend_block(
                    states[number],
                    entry[0],
                    entry[1],
                    entry[2],
                    key_piece,
                    value_piece,
                    seg_piece,
                    start,
                )
                for number, entry in enumerate(query_sets)
            )
        )

    def fold(states, piece, start):
        key_piece, value_piece, seg_piece = piece
        rows = key_piece.shape[0]
        width = 512

        def loop_step(index, carried):
            offset = index * width
            return apply_all(
                carried,
                lax.dynamic_slice_in_dim(key_piece, offset, width, 0),
                lax.dynamic_slice_in_dim(value_piece, offset, width, 0),
                lax.dynamic_slice_in_dim(seg_piece, offset, width, 0),
                offset,
            )

        return lax.fori_loop(0, rows // width, loop_step, states)

    return fold


def start_state(query_heads):
    tok_rows, groups, repeat_factor, head_size = query_heads.shape
    return (
        jnp.full((groups, repeat_factor, tok_rows), NEG_FILL, jnp.float32),
        jnp.zeros((groups, repeat_factor, tok_rows), jnp.float32),
        jnp.zeros((groups, repeat_factor, tok_rows, head_size), jnp.float32),
    )


def finish(state):
    _, weight_total, totals = state
    result = totals / weight_total[..., None]
    groups, repeat_factor, tok_rows, head_size = result.shape
    return (
        jnp.transpose(result, (2, 0, 1, 3))
        .reshape(tok_rows, groups * repeat_factor * head_size)
        .astype(jnp.bfloat16)
    )


def per_device_general(queries, key_matrix, value_matrix, segment_ids):
    head_size = HEAD_WIDTH
    block_rows = segment_ids.shape[0]
    groups = key_matrix.shape[1] // head_size
    repeat_factor = queries.shape[1] // head_size // groups
    position = lax.axis_index("seq")
    query_pos = position * block_rows + jnp.arange(block_rows, dtype=jnp.int32)
    query_sets = (
        (queries.reshape(block_rows, groups, repeat_factor, head_size), query_pos, segment_ids),
    )
    fold = build_fold(query_sets)
    states = tuple((start_state(entry[0]) for entry in query_sets))
    states = fold(
        states,
        (
            lax.all_gather(key_matrix, "seq", axis=0, tiled=True),
            lax.all_gather(value_matrix, "seq", axis=0, tiled=True),
            lax.all_gather(segment_ids, "seq", axis=0, tiled=True),
        ),
        jnp.int32(0),
    )
    return finish(states[0])


def paired_axis(count):
    return 8 <= count <= 16 and count & (count - 1) == 0


def suits(count, queries, key_matrix):
    tokens, lanes = key_matrix.shape
    return (
        paired_axis(count)
        and tokens == lanes == 2 * HEAD_WIDTH
        and queries.shape[1] % lanes == 0
    )


def per_device_any(count, queries, key_matrix, value_matrix, segment_ids):
    body = functools.partial(per_device, count)
    if not suits(count, queries, key_matrix):
        body = per_device_general
    return body(queries, key_matrix, value_matrix, segment_ids)


def solution(mesh):
    count = mesh.shape["seq"]
    in_specs = (P(("sweep", "seq"), "head"),) * 3 + (P(("sweep", "seq")),)
    return jax.shard_map(
        functools.partial(per_device_any, count),
        mesh=mesh, in_specs=in_specs, out_specs=P(("sweep", "seq"), "head"), check_vma=False,
    )
```

```python
import functools
import math

import jax
import jax.numpy as jnp
from jax import lax
from jax.experimental import pallas as pl
from jax.experimental.pallas import tpu as pltpu
from jax.sharding import PartitionSpec as P


HEAD_WIDTH = 64
NEG_FILL = -1e30
SEG_ROWS = 8
SMALL_VMEM = 1 << 20
VMEM_LIMIT = 16 << 20
VMEM = pl.BlockSpec(memory_space=pltpu.VMEM)
HBM = pl.BlockSpec(memory_space=pltpu.HBM)


def in_hbm(array):
    return pltpu.with_memory_space_constraint(array, pltpu.HBM)


def pack_kernel(k_ref, v_ref, seg_ref, out_ref, seg_buf, sems):
    tokens = k_ref.shape[0]
    copies = [
        pltpu.make_async_copy(seg_ref, seg_buf, sems.at[0]),
        pltpu.make_async_copy(k_ref, out_ref.at[:tokens], sems.at[1]),
        pltpu.make_async_copy(v_ref, out_ref.at[tokens : 2 * tokens], sems.at[2]),
    ]
    for copy in copies:
        copy.start()
    copies[0].wait()
    row = jnp.broadcast_to(seg_buf[...].astype(jnp.float32), (SEG_ROWS, tokens))
    out_ref[2 * tokens :] = row.astype(jnp.bfloat16)
    copies[1].wait()
    copies[2].wait()


def pack(key_matrix, value_matrix, seg_row):
    tokens, lanes = key_matrix.shape
    return pl.pallas_call(
        pack_kernel,
        out_shape=pltpu.VMEM((2 * tokens + SEG_ROWS, lanes), key_matrix.dtype),
        in_specs=[HBM] * 3,
        out_specs=VMEM,
        scratch_shapes=[pltpu.VMEM((1, tokens), jnp.int32), pltpu.SemaphoreType.DMA((3,))],
        compiler_params=pltpu.CompilerParams(vmem_limit_bytes=SMALL_VMEM),
        name="pack",
    )(in_hbm(key_matrix), in_hbm(value_matrix), in_hbm(seg_row))


def joined(pieces, first, tokens):
    parts = [piece[first : first + tokens] for piece in pieces]
    return parts[0] if len(parts) == 1 else jnp.concatenate(parts, axis=0)


def seg_grid(piece, tokens):
    line = piece[2 * tokens :].astype(jnp.float32)[0:1]
    return jnp.broadcast_to(line, (tokens, tokens))


def bias_of(me, step, piece, query_seg):
    tokens = query_seg.shape[0]
    key_seg = seg_grid(piece, tokens)
    if step == 0:
        row = lax.broadcasted_iota(jnp.int32, (tokens, tokens), 0)
        col = lax.broadcasted_iota(jnp.int32, (tokens, tokens), 1)
        seen = ((key_seg == query_seg) | (key_seg == 0.0)) & (col <= row)
    else:
        if step == 1:
            key_seg = jnp.where((me ^ step) < me, key_seg, -1.0)
        seen = (key_seg == query_seg) | (key_seg == 0.0)
    return jnp.where(seen, 0.0, NEG_FILL)


def folded(values, tokens, op):
    parts = [values[:, at : at + tokens] for at in range(0, values.shape[1], tokens)]
    return functools.reduce(op, parts)


def attend(me, blocks, query_seg, q_all, scores, heads, factor, before, after):
    tokens = query_seg.shape[0]
    query_rows = q_all[...]
    biases, value_blocks = [], []
    for number, block in enumerate(blocks):
        members = [piece for _, piece in block]
        scores[number, :, : len(block) * tokens] = lax.dot_general(
            query_rows, joined(members, 0, tokens), (((1,), (1,)), ((), ())),
            preferred_element_type=jnp.float32,
        )
        parts = [bias_of(me, step, piece, query_seg) for step, piece in block]
        biases.append(parts[0] if len(parts) == 1 else jnp.concatenate(parts, axis=1))
        value_blocks.append(joined(members, tokens, tokens))
    for head in range(heads):
        rows = slice(head * tokens, (head + 1) * tokens)
        state = before(rows)
        masked = []
        high = None if state is None else state[0]
        for number, block in enumerate(blocks):
            part = scores[number, rows, : len(block) * tokens] + biases[number]
            masked.append(part)
            part = folded(part, tokens, jnp.maximum)
            high = part if high is None else jnp.maximum(high, part)
        top = jnp.max(high, axis=1, keepdims=True)
        total = mixed = None
        if state is not None:
            rescale = jnp.exp2((state[0] - top) * factor)
            total, mixed = state[1] * rescale, state[2] * rescale
        for part, value_block in zip(masked, value_blocks):
            weights = jnp.exp2((part - top) * factor)
            share = folded(weights, tokens, jnp.add)
            total = share if total is None else total + share
            product = jnp.dot(
                weights.astype(jnp.bfloat16), value_block, preferred_element_type=jnp.float32
            )
            mixed = product if mixed is None else mixed + product
        after(head, rows, top, total, mixed)


class Output:
    def __init__(self, repeat, width, lanes, buf, hbm, sems):
        self.repeat, self.width, self.lanes = repeat, width, lanes
        self.buf, self.hbm, self.sems = buf, hbm, sems
        self.head, self.whole, self.copies = 0, None, []

    def add(self, value):
        slot = self.head % (self.lanes // self.width)
        shift = (slot * self.width - self.head // self.repeat * self.width) % self.lanes
        if shift:
            value = pltpu.roll(value, shift, 1)
        if slot:
            lane = lax.broadcasted_iota(jnp.int32, value.shape, 1)
            value = jnp.where(lane >= slot * self.width, value, self.whole)
        self.whole = value
        self.head += 1
        if (slot + 1) * self.width == self.lanes:
            tile = len(self.copies)
            where = slice(tile * self.lanes, (tile + 1) * self.lanes)
            self.buf[:, where] = value.astype(jnp.bfloat16)
            copy = pltpu.make_async_copy(self.buf.at[:, where], self.hbm.at[:, where], self.sems.at[tile])
            copy.start()
            self.copies.append(copy)

    def finish(self):
        for copy in self.copies:
            copy.wait()


def normal(total, mixed):
    return mixed * (1.0 / jnp.sum(total, axis=1, keepdims=True))


def paired(items):
    return [items[at : at + 2] for at in range(0, len(items), 2)]


def seen_steps(pair, count):
    return [step for step in range(2, count, 2) if pair ^ (step >> 1) < pair]


def prep_kernel(groups, repeat, q_hbm, own, q_all, seg_ref, q_buf, sems):
    tokens, columns = q_buf.shape
    lanes = q_all.shape[1]
    width = lanes // groups
    copies = [
        pltpu.make_async_copy(q_hbm.at[:, at : at + lanes], q_buf.at[:, at : at + lanes], sems.at[at // lanes])
        for at in range(0, columns, lanes)
    ]
    for copy in copies:
        copy.start()
    seg_ref[...] = jnp.transpose(seg_grid(own, tokens))
    lane = lax.broadcasted_iota(jnp.int32, (tokens, lanes), 1)
    for head in range(groups * repeat):
        group = head // repeat
        first = head * width // lanes * lanes
        if first == head * width:
            copies[first // lanes].wait()
        tile = q_buf[:, first : first + lanes].astype(jnp.float32)
        shift = (group * width - (head * width - first)) % lanes
        if shift:
            tile = pltpu.roll(tile, shift, 1)
        keep = (lane >= group * width) & (lane < (group + 1) * width)
        q_all[head * tokens : (head + 1) * tokens, :] = jnp.where(keep, tile, 0.0).astype(jnp.bfloat16)


def near_steps(count):
    return [0, 1] + list(range(2, count, 2)) + [count - 1]


def far_steps(count):
    return list(range(3, count - 1, 2))


def near_kernel(groups, repeat, count, *refs):
    steps = near_steps(count)
    q_all, seg_ref, pieces = refs[0], refs[1], dict(zip(steps, refs[2 : 2 + len(steps)]))
    top_ref, sum_ref, mix_ref, out_hbm, out_buf, scores, sems = refs[2 + len(steps) :]
    lanes = q_all.shape[1]
    tokens = seg_ref.shape[0]
    width = lanes // groups
    heads = groups * repeat
    factor = math.log2(math.e) / math.sqrt(width)
    me = lax.axis_index("seq")
    query_seg = seg_ref[...]

    for pair in range(count // 2):

        @pl.when(me // 2 == pair)
        def _(pair=pair):
            early = seen_steps(pair, count)
            chosen = [step for step in steps if step < 2 or step & -2 in early]
            blocks = paired([(step, pieces[step]) for step in chosen])
            output = Output(repeat, width, lanes, out_buf, out_hbm, sems)

            def after(head, rows, top, total, mixed):
                if early:
                    top_ref[rows, :] = jnp.broadcast_to(top, (tokens, lanes))
                    sum_ref[rows, :] = total
                    mix_ref[rows, :] = mixed
                else:
                    output.add(normal(total, mixed))

            attend(me, blocks, query_seg, q_all, scores, heads, factor, lambda rows: None, after)
            output.finish()


def far_kernel(groups, repeat, count, *refs):
    steps = far_steps(count)
    q_all, seg_ref, top_ref, sum_ref, mix_ref, out_in = refs[:6]
    pieces = dict(zip(steps, refs[6 : 6 + len(steps)]))
    out_hbm, out_buf, scores, sems = refs[6 + len(steps) :]
    del out_in
    lanes = q_all.shape[1]
    width = lanes // groups
    heads = groups * repeat
    factor = math.log2(math.e) / math.sqrt(width)
    me = lax.axis_index("seq")

    for pair in range(1, count // 2):

        @pl.when(me // 2 == pair)
        def _(pair=pair):
            early = seen_steps(pair, count)
            blocks = paired([(step, pieces[step]) for step in steps if step & -2 in early])
            output = Output(repeat, width, lanes, out_buf, out_hbm, sems)

            def before(rows):
                return top_ref[rows, :], sum_ref[rows, :], mix_ref[rows, :]

            def after(head, rows, top, total, mixed):
                output.add(normal(total, mixed))

            attend(me, blocks, seg_ref[...], q_all, scores, heads, factor, before, after)
            output.finish()


def partners(count, cores, step, mask):
    def needs(i):
        return step < 2 or step % 2 == 0 or (i ^ step) // 2 < i // 2

    pairs = []
    for i in range(count):
        for core in range(cores):
            across = needs(i) or needs(i ^ mask)
            other = (i ^ mask) * cores + core if across else i * cores + (core ^ 1)
            pairs.append((i * cores + core, other))
    return pairs


def plan_of(count):
    column = [count - 2] + list(range(2, count - 2, 2))
    return [(step, 0, step) for step in column] + [(1, 0, 1)] + [(step + 1, step, 1) for step in column]


def per_device(count, cores, queries, key_matrix, value_matrix, segment_ids):
    tokens, lanes = key_matrix.shape
    groups = lanes // HEAD_WIDTH
    repeat = queries.shape[1] // HEAD_WIDTH // groups
    heads = groups * repeat
    plan = plan_of(count)
    held = {0: pack(key_matrix, value_matrix, segment_ids.reshape(1, tokens))}
    for step, source, mask in plan:
        held[step] = lax.ppermute(held[source], ("seq", "head"), partners(count, cores, step, mask))
    near = near_steps(count)
    far = far_steps(count)
    row_shape = (heads * tokens, lanes)
    score_shape = (heads * tokens, 2 * tokens)
    tiles = queries.shape[1] // lanes
    q_all, query_seg = pl.pallas_call(
        functools.partial(prep_kernel, groups, repeat),
        out_shape=[
            pltpu.VMEM(row_shape, jnp.bfloat16),
            pltpu.VMEM((tokens, tokens), jnp.float32),
        ],
        in_specs=[HBM, VMEM],
        out_specs=[VMEM] * 2,
        scratch_shapes=[
            pltpu.VMEM(queries.shape, queries.dtype),
            pltpu.SemaphoreType.DMA((tiles,)),
        ],
        compiler_params=pltpu.CompilerParams(vmem_limit_bytes=SMALL_VMEM),
        name="prep",
    )(in_hbm(queries), held[0])
    top, total, mixed, out = pl.pallas_call(
        functools.partial(near_kernel, groups, repeat, count),
        out_shape=[
            pltpu.VMEM(row_shape, jnp.float32),
            pltpu.VMEM(row_shape, jnp.float32),
            pltpu.VMEM(row_shape, jnp.float32),
            pltpu.HBM(queries.shape, queries.dtype),
        ],
        in_specs=[VMEM] * (2 + len(near)),
        out_specs=[VMEM] * 3 + [HBM],
        scratch_shapes=[
            pltpu.VMEM(queries.shape, queries.dtype),
            pltpu.VMEM(((len(near) + 1) // 2,) + score_shape, jnp.float32),
            pltpu.SemaphoreType.DMA((tiles,)),
        ],
        compiler_params=pltpu.CompilerParams(vmem_limit_bytes=VMEM_LIMIT),
        name="near",
    )(q_all, query_seg, *[held[step] for step in near])
    return pl.pallas_call(
        functools.partial(far_kernel, groups, repeat, count),
        out_shape=pltpu.HBM(queries.shape, queries.dtype),
        in_specs=[VMEM] * 5 + [HBM] + [VMEM] * len(far),
        out_specs=HBM,
        scratch_shapes=[
            pltpu.VMEM(queries.shape, queries.dtype),
            pltpu.VMEM(((len(far) + 1) // 2,) + score_shape, jnp.float32),
            pltpu.SemaphoreType.DMA((tiles,)),
        ],
        input_output_aliases={5: 0},
        compiler_params=pltpu.CompilerParams(vmem_limit_bytes=VMEM_LIMIT),
        name="far",
    )(q_all, query_seg, top, total, mixed, out, *[held[step] for step in far])


def attend_block(state, query_heads, query_pos, query_seg, key_blk, value_blk, seg_blk, key_start):
    run_max, weight_total, totals = state
    groups = query_heads.shape[1]
    head_size = query_heads.shape[3]
    count = key_blk.shape[0]
    key_pos = key_start + jnp.arange(count, dtype=jnp.int32)
    visible = (key_pos[None, :] <= query_pos[:, None]) & (
        (seg_blk[None, :] == query_seg[:, None]) | (seg_blk[None, :] == 0)
    )

    def update(unused):
        logit_scores = jnp.einsum(
            "opez,hpz->peoh",
            query_heads,
            key_blk.reshape(count, groups, head_size),
            preferred_element_type=jnp.float32,
        ) * (1.0 / math.sqrt(head_size))
        logit_scores = jnp.where(visible, logit_scores, NEG_FILL)
        new_max = jnp.maximum(run_max, jnp.max(logit_scores, axis=-1))
        weights = jnp.where(visible, jnp.exp(logit_scores - new_max[..., None]), 0.0)
        rescale = jnp.exp(run_max - new_max)
        new_sum = weight_total * rescale + jnp.sum(weights, axis=-1)
        mixed_output = jnp.einsum(
            "omhy,yoc->omhc",
            weights.astype(jnp.bfloat16),
            value_blk.reshape(count, groups, head_size),
            preferred_element_type=jnp.float32,
        )
        return (new_max, new_sum, totals * rescale[..., None] + mixed_output)

    def keep(unused):
        return state

    return lax.cond(jnp.any(visible), update, keep, 0)


def build_fold(query_sets):

    def apply_all(states, key_piece, value_piece, seg_piece, start):
        return tuple(
            (
                attend_block(
                    states[number],
                    entry[0],
                    entry[1],
                    entry[2],
                    key_piece,
                    value_piece,
                    seg_piece,
                    start,
                )
                for number, entry in enumerate(query_sets)
            )
        )

    def fold(states, piece, start):
        key_piece, value_piece, seg_piece = piece
        rows = key_piece.shape[0]
        width = 512

        def loop_step(index, carried):
            offset = index * width
            return apply_all(
                carried,
                lax.dynamic_slice_in_dim(key_piece, offset, width, 0),
                lax.dynamic_slice_in_dim(value_piece, offset, width, 0),
                lax.dynamic_slice_in_dim(seg_piece, offset, width, 0),
                offset,
            )

        return lax.fori_loop(0, rows // width, loop_step, states)

    return fold


def start_state(query_heads):
    tok_rows, groups, repeat_factor, head_size = query_heads.shape
    return (
        jnp.full((groups, repeat_factor, tok_rows), NEG_FILL, jnp.float32),
        jnp.zeros((groups, repeat_factor, tok_rows), jnp.float32),
        jnp.zeros((groups, repeat_factor, tok_rows, head_size), jnp.float32),
    )


def finish(state):
    _, weight_total, totals = state
    result = totals / weight_total[..., None]
    groups, repeat_factor, tok_rows, head_size = result.shape
    return (
        jnp.transpose(result, (2, 0, 1, 3))
        .reshape(tok_rows, groups * repeat_factor * head_size)
        .astype(jnp.bfloat16)
    )


def per_device_general(queries, key_matrix, value_matrix, segment_ids):
    head_size = HEAD_WIDTH
    block_rows = segment_ids.shape[0]
    groups = key_matrix.shape[1] // head_size
    repeat_factor = queries.shape[1] // head_size // groups
    position = lax.axis_index("seq")
    query_pos = position * block_rows + jnp.arange(block_rows, dtype=jnp.int32)
    query_sets = (
        (queries.reshape(block_rows, groups, repeat_factor, head_size), query_pos, segment_ids),
    )
    fold = build_fold(query_sets)
    states = tuple((start_state(entry[0]) for entry in query_sets))
    states = fold(
        states,
        (
            lax.all_gather(key_matrix, "seq", axis=0, tiled=True),
            lax.all_gather(value_matrix, "seq", axis=0, tiled=True),
            lax.all_gather(segment_ids, "seq", axis=0, tiled=True),
        ),
        jnp.int32(0),
    )
    return finish(states[0])


def paired_axis(count):
    return 8 <= count <= 16 and count & (count - 1) == 0


def suits(count, cores, queries, key_matrix):
    tokens, lanes = key_matrix.shape
    return (
        paired_axis(count)
        and cores == 2
        and tokens == lanes == 2 * HEAD_WIDTH
        and queries.shape[1] % lanes == 0
    )


def per_device_any(count, cores, queries, key_matrix, value_matrix, segment_ids):
    body = functools.partial(per_device, count, cores)
    if not suits(count, cores, queries, key_matrix):
        body = per_device_general
    return body(queries, key_matrix, value_matrix, segment_ids)


def solution(mesh):
    count = mesh.shape["seq"]
    in_specs = (P(("sweep", "seq"), "head"),) * 3 + (P(("sweep", "seq")),)
    return jax.shard_map(
        functools.partial(per_device_any, count, mesh.shape["head"]),
        mesh=mesh, in_specs=in_specs, out_specs=P(("sweep", "seq"), "head"), check_vma=False,
    )
```

```python
import functools
import math

import jax
import jax.numpy as jnp
from jax import lax
from jax.experimental import pallas as pl
from jax.experimental.pallas import tpu as pltpu
from jax.sharding import PartitionSpec as P


HEAD_WIDTH = 64
NEG_FILL = -1e30
SEG_ROWS = 8
SMALL_VMEM = 1 << 20
VMEM_LIMIT = 16 << 20
VMEM = pl.BlockSpec(memory_space=pltpu.VMEM)
HBM = pl.BlockSpec(memory_space=pltpu.HBM)


def in_hbm(array):
    return pltpu.with_memory_space_constraint(array, pltpu.HBM)


def pack_kernel(k_ref, v_ref, seg_ref, out_ref, seg_buf, sems):
    tokens = k_ref.shape[0]
    copies = [
        pltpu.make_async_copy(seg_ref, seg_buf, sems.at[0]),
        pltpu.make_async_copy(k_ref, out_ref.at[:tokens], sems.at[1]),
        pltpu.make_async_copy(v_ref, out_ref.at[tokens : 2 * tokens], sems.at[2]),
    ]
    for copy in copies:
        copy.start()
    copies[0].wait()
    row = jnp.broadcast_to(seg_buf[...].astype(jnp.float32), (SEG_ROWS, tokens))
    out_ref[2 * tokens :] = row.astype(jnp.bfloat16)
    copies[1].wait()
    copies[2].wait()


def pack(key_matrix, value_matrix, seg_row):
    tokens, lanes = key_matrix.shape
    return pl.pallas_call(
        pack_kernel,
        out_shape=pltpu.VMEM((2 * tokens + SEG_ROWS, lanes), key_matrix.dtype),
        in_specs=[HBM] * 3,
        out_specs=VMEM,
        scratch_shapes=[pltpu.VMEM((1, tokens), jnp.int32), pltpu.SemaphoreType.DMA((3,))],
        compiler_params=pltpu.CompilerParams(vmem_limit_bytes=SMALL_VMEM),
        name="pack",
    )(in_hbm(key_matrix), in_hbm(value_matrix), in_hbm(seg_row))


def joined(pieces, first, tokens):
    parts = [piece[first : first + tokens] for piece in pieces]
    return parts[0] if len(parts) == 1 else jnp.concatenate(parts, axis=0)


def seg_grid(piece, tokens):
    line = piece[2 * tokens :].astype(jnp.float32)[0:1]
    return jnp.broadcast_to(line, (tokens, tokens))


def bias_of(me, step, piece, query_seg):
    tokens = query_seg.shape[0]
    key_seg = seg_grid(piece, tokens)
    if step == 0:
        row = lax.broadcasted_iota(jnp.int32, (tokens, tokens), 0)
        col = lax.broadcasted_iota(jnp.int32, (tokens, tokens), 1)
        seen = ((key_seg == query_seg) | (key_seg == 0.0)) & (col <= row)
    else:
        if step == 1:
            key_seg = jnp.where((me ^ step) < me, key_seg, -1.0)
        seen = (key_seg == query_seg) | (key_seg == 0.0)
    return jnp.where(seen, 0.0, NEG_FILL)


def folded(values, tokens, op):
    parts = [values[:, at : at + tokens] for at in range(0, values.shape[1], tokens)]
    return functools.reduce(op, parts)


def attend(me, blocks, query_seg, q_all, scores, heads, factor, before, after):
    tokens = query_seg.shape[0]
    query_rows = q_all[...]
    biases, value_blocks = [], []
    for number, block in enumerate(blocks):
        members = [piece for _, piece in block]
        scores[number, :, : len(block) * tokens] = lax.dot_general(
            query_rows, joined(members, 0, tokens), (((1,), (1,)), ((), ())),
            preferred_element_type=jnp.float32,
        )
        parts = [bias_of(me, step, piece, query_seg) for step, piece in block]
        biases.append(parts[0] if len(parts) == 1 else jnp.concatenate(parts, axis=1))
        value_blocks.append(joined(members, tokens, tokens))
    for head in range(heads):
        rows = slice(head * tokens, (head + 1) * tokens)
        state = before(rows)
        masked = []
        high = None if state is None else state[0]
        for number, block in enumerate(blocks):
            part = scores[number, rows, : len(block) * tokens] + biases[number]
            masked.append(part)
            part = folded(part, tokens, jnp.maximum)
            high = part if high is None else jnp.maximum(high, part)
        top = jnp.max(high, axis=1, keepdims=True)
        total = mixed = None
        if state is not None:
            rescale = jnp.exp2((state[0] - top) * factor)
            total, mixed = state[1] * rescale, state[2] * rescale
        for part, value_block in zip(masked, value_blocks):
            weights = jnp.exp2((part - top) * factor)
            share = folded(weights, tokens, jnp.add)
            total = share if total is None else total + share
            product = jnp.dot(
                weights.astype(jnp.bfloat16), value_block, preferred_element_type=jnp.float32
            )
            mixed = product if mixed is None else mixed + product
        after(head, rows, top, total, mixed)


class Output:
    def __init__(self, repeat, width, lanes, buf, hbm, sems):
        self.repeat, self.width, self.lanes = repeat, width, lanes
        self.buf, self.hbm, self.sems = buf, hbm, sems
        self.head, self.whole, self.copies = 0, None, []

    def add(self, value):
        slot = self.head % (self.lanes // self.width)
        shift = (slot * self.width - self.head // self.repeat * self.width) % self.lanes
        if shift:
            value = pltpu.roll(value, shift, 1)
        if slot:
            lane = lax.broadcasted_iota(jnp.int32, value.shape, 1)
            value = jnp.where(lane >= slot * self.width, value, self.whole)
        self.whole = value
        self.head += 1
        if (slot + 1) * self.width == self.lanes:
            tile = len(self.copies)
            where = slice(tile * self.lanes, (tile + 1) * self.lanes)
            self.buf[:, where] = value.astype(jnp.bfloat16)
            copy = pltpu.make_async_copy(self.buf.at[:, where], self.hbm.at[:, where], self.sems.at[tile])
            copy.start()
            self.copies.append(copy)

    def finish(self):
        for copy in self.copies:
            copy.wait()


def normal(total, mixed):
    return mixed * (1.0 / jnp.sum(total, axis=1, keepdims=True))


def paired(items):
    return [items[at : at + 2] for at in range(0, len(items), 2)]


def seen_steps(pair, count):
    return [step for step in range(2, count, 2) if pair ^ (step >> 1) < pair]


def prep_kernel(groups, repeat, q_hbm, own, q_all, seg_ref, q_buf, sems):
    tokens, columns = q_buf.shape
    lanes = q_all.shape[1]
    width = lanes // groups
    copies = [
        pltpu.make_async_copy(q_hbm.at[:, at : at + lanes], q_buf.at[:, at : at + lanes], sems.at[at // lanes])
        for at in range(0, columns, lanes)
    ]
    for copy in copies:
        copy.start()
    seg_ref[...] = jnp.transpose(seg_grid(own, tokens))
    lane = lax.broadcasted_iota(jnp.int32, (tokens, lanes), 1)
    for head in range(groups * repeat):
        group = head // repeat
        first = head * width // lanes * lanes
        if first == head * width:
            copies[first // lanes].wait()
        tile = q_buf[:, first : first + lanes].astype(jnp.float32)
        shift = (group * width - (head * width - first)) % lanes
        if shift:
            tile = pltpu.roll(tile, shift, 1)
        keep = (lane >= group * width) & (lane < (group + 1) * width)
        q_all[head * tokens : (head + 1) * tokens, :] = jnp.where(keep, tile, 0.0).astype(jnp.bfloat16)


def stages_of(count):
    forwarded = [step for step, _, _ in plan_of(count) if step > 1 and step % 2]
    return [[0, 1] + list(range(2, count, 2)), forwarded[:-1], forwarded[-1:]]


def stage_kernel(groups, repeat, count, number, *refs):
    stages = stages_of(count)
    steps = stages[number]
    q_all, seg_ref, pieces = refs[0], refs[1], dict(zip(steps, refs[2 : 2 + len(steps)]))
    top_ref, sum_ref, mix_ref, out_hbm, out_buf, scores, sems = refs[-7:]
    lanes = q_all.shape[1]
    tokens = seg_ref.shape[0]
    width = lanes // groups
    heads = groups * repeat
    factor = math.log2(math.e) / math.sqrt(width)
    me = lax.axis_index("seq")

    for pair in range(count // 2):
        early = seen_steps(pair, count)
        seen = [[step for step in stage if step < 2 or step & -2 in early] for stage in stages]
        if not seen[number]:
            continue

        @pl.when(me // 2 == pair)
        def _(seen=seen):
            more = any(seen[number + 1 :])
            output = Output(repeat, width, lanes, out_buf, out_hbm, sems)

            def before(rows):
                if number == 0:
                    return None
                return top_ref[rows, :], sum_ref[rows, :], mix_ref[rows, :]

            def after(head, rows, top, total, mixed):
                if more:
                    top_ref[rows, :] = jnp.broadcast_to(top, (tokens, lanes))
                    sum_ref[rows, :] = total
                    mix_ref[rows, :] = mixed
                else:
                    output.add(normal(total, mixed))

            blocks = paired([(step, pieces[step]) for step in seen[number]])
            attend(me, blocks, seg_ref[...], q_all, scores, heads, factor, before, after)
            output.finish()


def stage_call(groups, repeat, count, number, queries, q_all, query_seg, pieces, carried):
    rows, lanes = q_all.shape
    tokens = query_seg.shape[0]
    state = pltpu.VMEM((rows, lanes), jnp.float32)
    first = 2 + len(pieces)
    return pl.pallas_call(
        functools.partial(stage_kernel, groups, repeat, count, number),
        out_shape=[state, state, state, pltpu.HBM(queries.shape, queries.dtype)],
        in_specs=[VMEM] * first + ([VMEM] * 3 + [HBM] if carried else []),
        out_specs=[VMEM] * 3 + [HBM],
        scratch_shapes=[
            pltpu.VMEM((tokens, queries.shape[1]), queries.dtype),
            pltpu.VMEM(((len(pieces) + 1) // 2, rows, 2 * tokens), jnp.float32),
            pltpu.SemaphoreType.DMA((queries.shape[1] // lanes,)),
        ],
        input_output_aliases={first + at: at for at in range(4)} if carried else {},
        compiler_params=pltpu.CompilerParams(vmem_limit_bytes=VMEM_LIMIT),
    )(q_all, query_seg, *pieces, *carried)


def partners(count, cores, step, source, mask):
    def needs(i):
        return source == 0 or (i ^ step) // 2 < i // 2

    pairs = []
    for i in range(count):
        for core in range(cores):
            across = needs(i) or needs(i ^ mask)
            other = (i ^ mask) * cores + core if across else i * cores + (core ^ 1)
            pairs.append((i * cores + core, other))
    return pairs


def plan_of(count):
    column = [count - 2] + list(range(2, count - 2, 2))
    return [(step, 0, step) for step in column] + [(1, 0, 1)] + [(step + 1, step, 1) for step in column]


def per_device(count, cores, queries, key_matrix, value_matrix, segment_ids):
    tokens, lanes = key_matrix.shape
    groups = lanes // HEAD_WIDTH
    repeat = queries.shape[1] // HEAD_WIDTH // groups
    heads = groups * repeat
    plan = plan_of(count)
    held = {0: pack(key_matrix, value_matrix, segment_ids.reshape(1, tokens))}
    for step, source, mask in plan:
        held[step] = lax.ppermute(held[source], ("seq", "head"), partners(count, cores, step, source, mask))
    row_shape = (heads * tokens, lanes)
    tiles = queries.shape[1] // lanes
    q_all, query_seg = pl.pallas_call(
        functools.partial(prep_kernel, groups, repeat),
        out_shape=[
            pltpu.VMEM(row_shape, jnp.bfloat16),
            pltpu.VMEM((tokens, tokens), jnp.float32),
        ],
        in_specs=[HBM, VMEM],
        out_specs=[VMEM] * 2,
        scratch_shapes=[
            pltpu.VMEM(queries.shape, queries.dtype),
            pltpu.SemaphoreType.DMA((tiles,)),
        ],
        compiler_params=pltpu.CompilerParams(vmem_limit_bytes=SMALL_VMEM),
        name="prep",
    )(in_hbm(queries), held[0])
    carried = []
    for number, steps in enumerate(stages_of(count)):
        carried = stage_call(
            groups, repeat, count, number, queries, q_all, query_seg,
            [held[step] for step in steps], carried,
        )
    return carried[-1]


def attend_block(state, query_heads, query_pos, query_seg, key_blk, value_blk, seg_blk, key_start):
    run_max, weight_total, totals = state
    groups = query_heads.shape[1]
    head_size = query_heads.shape[3]
    count = key_blk.shape[0]
    key_pos = key_start + jnp.arange(count, dtype=jnp.int32)
    visible = (key_pos[None, :] <= query_pos[:, None]) & (
        (seg_blk[None, :] == query_seg[:, None]) | (seg_blk[None, :] == 0)
    )

    def update(unused):
        logit_scores = jnp.einsum(
            "opez,hpz->peoh",
            query_heads,
            key_blk.reshape(count, groups, head_size),
            preferred_element_type=jnp.float32,
        ) * (1.0 / math.sqrt(head_size))
        logit_scores = jnp.where(visible, logit_scores, NEG_FILL)
        new_max = jnp.maximum(run_max, jnp.max(logit_scores, axis=-1))
        weights = jnp.where(visible, jnp.exp(logit_scores - new_max[..., None]), 0.0)
        rescale = jnp.exp(run_max - new_max)
        new_sum = weight_total * rescale + jnp.sum(weights, axis=-1)
        mixed_output = jnp.einsum(
            "omhy,yoc->omhc",
            weights.astype(jnp.bfloat16),
            value_blk.reshape(count, groups, head_size),
            preferred_element_type=jnp.float32,
        )
        return (new_max, new_sum, totals * rescale[..., None] + mixed_output)

    def keep(unused):
        return state

    return lax.cond(jnp.any(visible), update, keep, 0)


def build_fold(query_sets):

    def apply_all(states, key_piece, value_piece, seg_piece, start):
        return tuple(
            (
                attend_block(
                    states[number],
                    entry[0],
                    entry[1],
                    entry[2],
                    key_piece,
                    value_piece,
                    seg_piece,
                    start,
                )
                for number, entry in enumerate(query_sets)
            )
        )

    def fold(states, piece, start):
        key_piece, value_piece, seg_piece = piece
        rows = key_piece.shape[0]
        width = 512

        def loop_step(index, carried):
            offset = index * width
            return apply_all(
                carried,
                lax.dynamic_slice_in_dim(key_piece, offset, width, 0),
                lax.dynamic_slice_in_dim(value_piece, offset, width, 0),
                lax.dynamic_slice_in_dim(seg_piece, offset, width, 0),
                offset,
            )

        return lax.fori_loop(0, rows // width, loop_step, states)

    return fold


def start_state(query_heads):
    tok_rows, groups, repeat_factor, head_size = query_heads.shape
    return (
        jnp.full((groups, repeat_factor, tok_rows), NEG_FILL, jnp.float32),
        jnp.zeros((groups, repeat_factor, tok_rows), jnp.float32),
        jnp.zeros((groups, repeat_factor, tok_rows, head_size), jnp.float32),
    )


def finish(state):
    _, weight_total, totals = state
    result = totals / weight_total[..., None]
    groups, repeat_factor, tok_rows, head_size = result.shape
    return (
        jnp.transpose(result, (2, 0, 1, 3))
        .reshape(tok_rows, groups * repeat_factor * head_size)
        .astype(jnp.bfloat16)
    )


def per_device_general(queries, key_matrix, value_matrix, segment_ids):
    head_size = HEAD_WIDTH
    block_rows = segment_ids.shape[0]
    groups = key_matrix.shape[1] // head_size
    repeat_factor = queries.shape[1] // head_size // groups
    position = lax.axis_index("seq")
    query_pos = position * block_rows + jnp.arange(block_rows, dtype=jnp.int32)
    query_sets = (
        (queries.reshape(block_rows, groups, repeat_factor, head_size), query_pos, segment_ids),
    )
    fold = build_fold(query_sets)
    states = tuple((start_state(entry[0]) for entry in query_sets))
    states = fold(
        states,
        (
            lax.all_gather(key_matrix, "seq", axis=0, tiled=True),
            lax.all_gather(value_matrix, "seq", axis=0, tiled=True),
            lax.all_gather(segment_ids, "seq", axis=0, tiled=True),
        ),
        jnp.int32(0),
    )
    return finish(states[0])


def paired_axis(count):
    return 8 <= count <= 16 and count & (count - 1) == 0


def suits(count, cores, queries, key_matrix):
    tokens, lanes = key_matrix.shape
    return (
        paired_axis(count)
        and cores == 2
        and tokens == lanes == 2 * HEAD_WIDTH
        and queries.shape[1] % lanes == 0
    )


def per_device_any(count, cores, queries, key_matrix, value_matrix, segment_ids):
    body = functools.partial(per_device, count, cores)
    if not suits(count, cores, queries, key_matrix):
        body = per_device_general
    return body(queries, key_matrix, value_matrix, segment_ids)


def solution(mesh):
    count = mesh.shape["seq"]
    in_specs = (P(("sweep", "seq"), "head"),) * 3 + (P(("sweep", "seq")),)
    return jax.shard_map(
        functools.partial(per_device_any, count, mesh.shape["head"]),
        mesh=mesh, in_specs=in_specs, out_specs=P(("sweep", "seq"), "head"), check_vma=False,
    )
```

```python
import functools
import math

import jax
import jax.numpy as jnp
from jax import lax
from jax.experimental import pallas as pl
from jax.experimental.pallas import tpu as pltpu
from jax.sharding import PartitionSpec as P


HEAD_WIDTH = 64
NEG_FILL = -1e30
SEG_ROWS = 8
SMALL_VMEM = 1 << 20
VMEM_LIMIT = 16 << 20
VMEM = pl.BlockSpec(memory_space=pltpu.VMEM)
HBM = pl.BlockSpec(memory_space=pltpu.HBM)


def in_hbm(array):
    return pltpu.with_memory_space_constraint(array, pltpu.HBM)


def pack_kernel(k_ref, v_ref, seg_ref, out_ref, seg_buf, sems):
    tokens = k_ref.shape[0]
    copies = [
        pltpu.make_async_copy(seg_ref, seg_buf, sems.at[0]),
        pltpu.make_async_copy(k_ref, out_ref.at[:tokens], sems.at[1]),
        pltpu.make_async_copy(v_ref, out_ref.at[tokens : 2 * tokens], sems.at[2]),
    ]
    for copy in copies:
        copy.start()
    copies[0].wait()
    row = jnp.broadcast_to(seg_buf[...].astype(jnp.float32), (SEG_ROWS, tokens))
    out_ref[2 * tokens :] = row.astype(jnp.bfloat16)
    copies[1].wait()
    copies[2].wait()


def pack(key_matrix, value_matrix, seg_row):
    tokens, lanes = key_matrix.shape
    return pl.pallas_call(
        pack_kernel,
        out_shape=pltpu.VMEM((2 * tokens + SEG_ROWS, lanes), key_matrix.dtype),
        in_specs=[HBM] * 3,
        out_specs=VMEM,
        scratch_shapes=[pltpu.VMEM((1, tokens), jnp.int32), pltpu.SemaphoreType.DMA((3,))],
        compiler_params=pltpu.CompilerParams(vmem_limit_bytes=SMALL_VMEM),
        name="pack",
    )(in_hbm(key_matrix), in_hbm(value_matrix), in_hbm(seg_row))


def joined(pieces, first, tokens):
    parts = [piece[first : first + tokens] for piece in pieces]
    return parts[0] if len(parts) == 1 else jnp.concatenate(parts, axis=0)


def seg_grid(piece, tokens):
    line = piece[2 * tokens :].astype(jnp.float32)[0:1]
    return jnp.broadcast_to(line, (tokens, tokens))


def bias_of(me, step, piece, query_seg):
    tokens = query_seg.shape[0]
    key_seg = seg_grid(piece, tokens)
    if step == 0:
        row = lax.broadcasted_iota(jnp.int32, (tokens, tokens), 0)
        col = lax.broadcasted_iota(jnp.int32, (tokens, tokens), 1)
        seen = ((key_seg == query_seg) | (key_seg == 0.0)) & (col <= row)
    else:
        if step == 1:
            key_seg = jnp.where((me ^ step) < me, key_seg, -1.0)
        seen = (key_seg == query_seg) | (key_seg == 0.0)
    return jnp.where(seen, 0.0, NEG_FILL)


def folded(values, tokens, op):
    parts = [values[:, at : at + tokens] for at in range(0, values.shape[1], tokens)]
    return functools.reduce(op, parts)


def attend(me, blocks, query_seg, q_all, scores, heads, factor, before, after):
    tokens = query_seg.shape[0]
    query_rows = q_all[...]
    biases, value_blocks = [], []
    for number, block in enumerate(blocks):
        members = [piece for _, piece in block]
        scores[number, :, : len(block) * tokens] = lax.dot_general(
            query_rows, joined(members, 0, tokens), (((1,), (1,)), ((), ())),
            preferred_element_type=jnp.float32,
        )
        parts = [bias_of(me, step, piece, query_seg) for step, piece in block]
        biases.append(parts[0] if len(parts) == 1 else jnp.concatenate(parts, axis=1))
        value_blocks.append(joined(members, tokens, tokens))
    for head in range(heads):
        rows = slice(head * tokens, (head + 1) * tokens)
        state = before(rows)
        masked = []
        high = None if state is None else state[0]
        for number, block in enumerate(blocks):
            part = scores[number, rows, : len(block) * tokens] + biases[number]
            masked.append(part)
            part = folded(part, tokens, jnp.maximum)
            high = part if high is None else jnp.maximum(high, part)
        top = jnp.max(high, axis=1, keepdims=True)
        total = mixed = None
        if state is not None:
            rescale = jnp.exp2((state[0] - top) * factor)
            total, mixed = state[1] * rescale, state[2] * rescale
        for part, value_block in zip(masked, value_blocks):
            weights = jnp.exp2((part - top) * factor)
            share = folded(weights, tokens, jnp.add)
            total = share if total is None else total + share
            product = jnp.dot(
                weights.astype(jnp.bfloat16), value_block, preferred_element_type=jnp.float32
            )
            mixed = product if mixed is None else mixed + product
        after(head, rows, top, total, mixed)


class Output:
    def __init__(self, repeat, width, lanes, buf, hbm, sems):
        self.repeat, self.width, self.lanes = repeat, width, lanes
        self.buf, self.hbm, self.sems = buf, hbm, sems
        self.head, self.whole, self.copies = 0, None, []

    def add(self, value):
        slot = self.head % (self.lanes // self.width)
        shift = (slot * self.width - self.head // self.repeat * self.width) % self.lanes
        if shift:
            value = pltpu.roll(value, shift, 1)
        if slot:
            lane = lax.broadcasted_iota(jnp.int32, value.shape, 1)
            value = jnp.where(lane >= slot * self.width, value, self.whole)
        self.whole = value
        self.head += 1
        if (slot + 1) * self.width == self.lanes:
            tile = len(self.copies)
            where = slice(tile * self.lanes, (tile + 1) * self.lanes)
            self.buf[:, where] = value.astype(jnp.bfloat16)
            copy = pltpu.make_async_copy(self.buf.at[:, where], self.hbm.at[:, where], self.sems.at[tile])
            copy.start()
            self.copies.append(copy)

    def finish(self):
        for copy in self.copies:
            copy.wait()


def normal(total, mixed):
    return mixed * (1.0 / jnp.sum(total, axis=1, keepdims=True))


def paired(items):
    return [items[at : at + 2] for at in range(0, len(items), 2)]


def seen_steps(pair, count):
    return [step for step in range(2, count, 2) if pair ^ (step >> 1) < pair]


def prep_kernel(groups, repeat, q_hbm, own, q_all, seg_ref, q_buf, sems):
    tokens, columns = q_buf.shape
    lanes = q_all.shape[1]
    width = lanes // groups
    copies = [
        pltpu.make_async_copy(q_hbm.at[:, at : at + lanes], q_buf.at[:, at : at + lanes], sems.at[at // lanes])
        for at in range(0, columns, lanes)
    ]
    for copy in copies:
        copy.start()
    seg_ref[...] = jnp.transpose(seg_grid(own, tokens))
    lane = lax.broadcasted_iota(jnp.int32, (tokens, lanes), 1)
    for head in range(groups * repeat):
        group = head // repeat
        first = head * width // lanes * lanes
        if first == head * width:
            copies[first // lanes].wait()
        tile = q_buf[:, first : first + lanes].astype(jnp.float32)
        shift = (group * width - (head * width - first)) % lanes
        if shift:
            tile = pltpu.roll(tile, shift, 1)
        keep = (lane >= group * width) & (lane < (group + 1) * width)
        q_all[head * tokens : (head + 1) * tokens, :] = jnp.where(keep, tile, 0.0).astype(jnp.bfloat16)


def stages_of(count):
    forwarded = [step for step, _, _ in plan_of(count) if step > 1 and step % 2]
    return [[0, 1] + list(range(2, count, 2)), forwarded[:-1], forwarded[-1:]]


def stage_kernel(groups, repeat, count, number, *refs):
    stages = stages_of(count)
    steps = stages[number]
    q_all, seg_ref, pieces = refs[0], refs[1], dict(zip(steps, refs[2 : 2 + len(steps)]))
    top_ref, sum_ref, mix_ref, out_hbm, out_buf, scores, sems = refs[-7:]
    lanes = q_all.shape[1]
    tokens = seg_ref.shape[0]
    width = lanes // groups
    heads = groups * repeat
    factor = math.log2(math.e) / math.sqrt(width)
    me = lax.axis_index("seq")

    for pair in range(count // 2):
        early = seen_steps(pair, count)
        seen = [[step for step in stage if step < 2 or step & -2 in early] for stage in stages]
        if not seen[number]:
            continue

        @pl.when(me // 2 == pair)
        def _(seen=seen, pair=pair):
            final = max(at for at in range(len(stages)) if seen[at])
            tested = final > 0 and all(step >> 1 != pair for step in seen[final])
            writes = number == final
            if tested:
                writes = number >= max(at for at in range(final) if seen[at])
            output = Output(repeat, width, lanes, out_buf, out_hbm, sems)

            def before(rows):
                if number == 0:
                    return None
                return top_ref[rows, :], sum_ref[rows, :], mix_ref[rows, :]

            def after(head, rows, top, total, mixed):
                if number < final:
                    top_ref[rows, :] = jnp.broadcast_to(top, (tokens, lanes))
                    sum_ref[rows, :] = total
                    mix_ref[rows, :] = mixed
                if writes:
                    output.add(normal(total, mixed))

            def run():
                blocks = paired([(step, pieces[step]) for step in seen[number]])
                attend(me, blocks, seg_ref[...], q_all, scores, heads, factor, before, after)
                output.finish()

            if number < final or not tested:
                run()
            else:
                parts = [bias_of(me, step, pieces[step], seg_ref[...]) for step in seen[number]]
                pl.when(jnp.max(functools.reduce(jnp.maximum, parts)) == 0.0)(run)


def stage_call(groups, repeat, count, number, queries, q_all, query_seg, pieces, carried):
    rows, lanes = q_all.shape
    tokens = query_seg.shape[0]
    state = pltpu.VMEM((rows, lanes), jnp.float32)
    first = 2 + len(pieces)
    return pl.pallas_call(
        functools.partial(stage_kernel, groups, repeat, count, number),
        out_shape=[state, state, state, pltpu.HBM(queries.shape, queries.dtype)],
        in_specs=[VMEM] * first + ([VMEM] * 3 + [HBM] if carried else []),
        out_specs=[VMEM] * 3 + [HBM],
        scratch_shapes=[
            pltpu.VMEM((tokens, queries.shape[1]), queries.dtype),
            pltpu.VMEM(((len(pieces) + 1) // 2, rows, 2 * tokens), jnp.float32),
            pltpu.SemaphoreType.DMA((queries.shape[1] // lanes,)),
        ],
        input_output_aliases={first + at: at for at in range(4)} if carried else {},
        compiler_params=pltpu.CompilerParams(vmem_limit_bytes=VMEM_LIMIT),
    )(q_all, query_seg, *pieces, *carried)


def partners(count, cores, step, source, mask):
    def needs(i):
        return source == 0 or (i ^ step) // 2 < i // 2

    pairs = []
    for i in range(count):
        for core in range(cores):
            across = needs(i) or needs(i ^ mask)
            other = (i ^ mask) * cores + core if across else i * cores + (core ^ 1)
            pairs.append((i * cores + core, other))
    return pairs


def plan_of(count):
    column = [count - 2] + list(range(2, count - 2, 2))
    onward = column[1:2] + column[:1] + column[2:]
    return [(step, 0, step) for step in column] + [(1, 0, 1)] + [(step + 1, step, 1) for step in onward]


def per_device(count, cores, queries, key_matrix, value_matrix, segment_ids):
    tokens, lanes = key_matrix.shape
    groups = lanes // HEAD_WIDTH
    repeat = queries.shape[1] // HEAD_WIDTH // groups
    heads = groups * repeat
    plan = plan_of(count)
    held = {0: pack(key_matrix, value_matrix, segment_ids.reshape(1, tokens))}
    for step, source, mask in plan:
        held[step] = lax.ppermute(held[source], ("seq", "head"), partners(count, cores, step, source, mask))
    row_shape = (heads * tokens, lanes)
    tiles = queries.shape[1] // lanes
    q_all, query_seg = pl.pallas_call(
        functools.partial(prep_kernel, groups, repeat),
        out_shape=[
            pltpu.VMEM(row_shape, jnp.bfloat16),
            pltpu.VMEM((tokens, tokens), jnp.float32),
        ],
        in_specs=[HBM, VMEM],
        out_specs=[VMEM] * 2,
        scratch_shapes=[
            pltpu.VMEM(queries.shape, queries.dtype),
            pltpu.SemaphoreType.DMA((tiles,)),
        ],
        compiler_params=pltpu.CompilerParams(vmem_limit_bytes=SMALL_VMEM),
        name="prep",
    )(in_hbm(queries), held[0])
    carried = []
    for number, steps in enumerate(stages_of(count)):
        carried = stage_call(
            groups, repeat, count, number, queries, q_all, query_seg,
            [held[step] for step in steps], carried,
        )
    return carried[-1]


def attend_block(state, query_heads, query_pos, query_seg, key_blk, value_blk, seg_blk, key_start):
    run_max, weight_total, totals = state
    groups = query_heads.shape[1]
    head_size = query_heads.shape[3]
    count = key_blk.shape[0]
    key_pos = key_start + jnp.arange(count, dtype=jnp.int32)
    visible = (key_pos[None, :] <= query_pos[:, None]) & (
        (seg_blk[None, :] == query_seg[:, None]) | (seg_blk[None, :] == 0)
    )

    def update(unused):
        logit_scores = jnp.einsum(
            "opez,hpz->peoh",
            query_heads,
            key_blk.reshape(count, groups, head_size),
            preferred_element_type=jnp.float32,
        ) * (1.0 / math.sqrt(head_size))
        logit_scores = jnp.where(visible, logit_scores, NEG_FILL)
        new_max = jnp.maximum(run_max, jnp.max(logit_scores, axis=-1))
        weights = jnp.where(visible, jnp.exp(logit_scores - new_max[..., None]), 0.0)
        rescale = jnp.exp(run_max - new_max)
        new_sum = weight_total * rescale + jnp.sum(weights, axis=-1)
        mixed_output = jnp.einsum(
            "omhy,yoc->omhc",
            weights.astype(jnp.bfloat16),
            value_blk.reshape(count, groups, head_size),
            preferred_element_type=jnp.float32,
        )
        return (new_max, new_sum, totals * rescale[..., None] + mixed_output)

    def keep(unused):
        return state

    return lax.cond(jnp.any(visible), update, keep, 0)


def build_fold(query_sets):

    def apply_all(states, key_piece, value_piece, seg_piece, start):
        return tuple(
            (
                attend_block(
                    states[number],
                    entry[0],
                    entry[1],
                    entry[2],
                    key_piece,
                    value_piece,
                    seg_piece,
                    start,
                )
                for number, entry in enumerate(query_sets)
            )
        )

    def fold(states, piece, start):
        key_piece, value_piece, seg_piece = piece
        rows = key_piece.shape[0]
        width = 512

        def loop_step(index, carried):
            offset = index * width
            return apply_all(
                carried,
                lax.dynamic_slice_in_dim(key_piece, offset, width, 0),
                lax.dynamic_slice_in_dim(value_piece, offset, width, 0),
                lax.dynamic_slice_in_dim(seg_piece, offset, width, 0),
                offset,
            )

        return lax.fori_loop(0, rows // width, loop_step, states)

    return fold


def start_state(query_heads):
    tok_rows, groups, repeat_factor, head_size = query_heads.shape
    return (
        jnp.full((groups, repeat_factor, tok_rows), NEG_FILL, jnp.float32),
        jnp.zeros((groups, repeat_factor, tok_rows), jnp.float32),
        jnp.zeros((groups, repeat_factor, tok_rows, head_size), jnp.float32),
    )


def finish(state):
    _, weight_total, totals = state
    result = totals / weight_total[..., None]
    groups, repeat_factor, tok_rows, head_size = result.shape
    return (
        jnp.transpose(result, (2, 0, 1, 3))
        .reshape(tok_rows, groups * repeat_factor * head_size)
        .astype(jnp.bfloat16)
    )


def per_device_general(queries, key_matrix, value_matrix, segment_ids):
    head_size = HEAD_WIDTH
    block_rows = segment_ids.shape[0]
    groups = key_matrix.shape[1] // head_size
    repeat_factor = queries.shape[1] // head_size // groups
    position = lax.axis_index("seq")
    query_pos = position * block_rows + jnp.arange(block_rows, dtype=jnp.int32)
    query_sets = (
        (queries.reshape(block_rows, groups, repeat_factor, head_size), query_pos, segment_ids),
    )
    fold = build_fold(query_sets)
    states = tuple((start_state(entry[0]) for entry in query_sets))
    states = fold(
        states,
        (
            lax.all_gather(key_matrix, "seq", axis=0, tiled=True),
            lax.all_gather(value_matrix, "seq", axis=0, tiled=True),
            lax.all_gather(segment_ids, "seq", axis=0, tiled=True),
        ),
        jnp.int32(0),
    )
    return finish(states[0])


def paired_axis(count):
    return 8 <= count <= 16 and count & (count - 1) == 0


def suits(count, cores, queries, key_matrix):
    tokens, lanes = key_matrix.shape
    return (
        paired_axis(count)
        and cores == 2
        and tokens == lanes == 2 * HEAD_WIDTH
        and queries.shape[1] % lanes == 0
    )


def per_device_any(count, cores, queries, key_matrix, value_matrix, segment_ids):
    body = functools.partial(per_device, count, cores)
    if not suits(count, cores, queries, key_matrix):
        body = per_device_general
    return body(queries, key_matrix, value_matrix, segment_ids)


def solution(mesh):
    count = mesh.shape["seq"]
    in_specs = (P(("sweep", "seq"), "head"),) * 3 + (P(("sweep", "seq")),)
    return jax.shard_map(
        functools.partial(per_device_any, count, mesh.shape["head"]),
        mesh=mesh, in_specs=in_specs, out_specs=P(("sweep", "seq"), "head"), check_vma=False,
    )
```
